8 devices in a mesh: hp: 1 (over z), cpo: 2 (over y), cp: 4 (over x, core).
Axes of the slice: x: 2, y: 2, z: 1, core: 2. Of those that a mesh axis runs over, the one named last changes fastest.
Arguments:
- q: bfloat16 [6144, 4, 128], P(('cpo', 'cp'), 'hp')
- k: bfloat16 [6144, 1, 128], P(('cpo', 'cp'), 'hp')
- v: bfloat16 [6144, 1, 128], P(('cpo', 'cp'), 'hp')
- out: bfloat16 [6144, 4, 128], P(('cpo', 'cp'), 'hp')
- dout: bfloat16 [6144, 4, 128], P(('cpo', 'cp'), 'hp')
- lse: float32 [6144, 4], P(('cpo', 'cp'), 'hp')
- cu_seqlens: int32 [9], replicated
Outputs:
- output 1: bfloat16 [6144, 4, 128], P(('cpo', 'cp'), 'hp')
- output 2: bfloat16 [6144, 1, 128], P(('cpo', 'cp'), 'hp')
- output 3: bfloat16 [6144, 1, 128], P(('cpo', 'cp'), 'hp')
All inputs are finite; a program needn't handle non-finite values.
Results may differ from the reference program's by a relative error of at most 0.001.
Values are sent between devices in bfloat16 or wider.
A program may use at most 1 GiB of HBM per device.

```python
import jax
import jax.numpy as jnp
from jax import lax

GQA = 4
HEAD = 128
TOKENS_DEV = 768
NCHUNK = 8
NDOC = 8

SEQ = NCHUNK * TOKENS_DEV


def _doc_ids(cu, seq):
    pos = jnp.arange(seq)
    return jnp.sum((cu[1:][None, :] <= pos[:, None]).astype(jnp.int32), axis=1)


def _draw_cu(key):
    key_base, key_pick, key_share = jax.random.split(key, 3)
    base_draw = jax.random.randint(key_base, (NDOC,), 13, 257).astype(jnp.uint32)
    cube_part = (base_draw * base_draw * base_draw) >> 13
    weights = cube_part * cube_part + 1
    pick_doc = jax.random.randint(key_pick, (), 0, NDOC)
    share_milli = jax.random.randint(key_share, (), 500, 701).astype(jnp.uint32)
    denom_milli = 1000 - share_milli
    rest_sum = jnp.sum(weights, dtype=jnp.uint32) - weights[pick_doc]
    weights = weights.at[pick_doc].set((rest_sum // denom_milli) * share_milli + (rest_sum % denom_milli) * share_milli // denom_milli)
    cum_sum = jnp.cumsum(weights, dtype=jnp.uint32)
    total_weight = cum_sum[-1]
    shift_steps = jnp.arange(32, dtype=jnp.uint32)
    shift_by = jnp.sum(((total_weight >> shift_steps) >> 15) > 0).astype(jnp.uint32)
    cum_small = cum_sum[:-1] >> shift_by
    total_small = total_weight >> shift_by
    room_tokens = SEQ - NDOC
    inner = cum_small * (room_tokens // total_small) + (cum_small * (room_tokens % total_small)) // total_small
    inner = inner.astype(jnp.int32) + jnp.arange(1, NDOC, dtype=jnp.int32)
    return jnp.concatenate([jnp.zeros((1,), jnp.int32), inner, jnp.full((1,), SEQ, jnp.int32)])


def _forward(q, k, v, doc):
    seq, hq, d = q.shape
    hk = k.shape[1]
    g = hq // hk
    c = TOKENS_DEV
    n = seq // c
    scale = d ** -0.5
    qc = q.astype(jnp.float32).reshape(n, c, hk, g, d)
    kc = k.astype(jnp.float32).reshape(n, c, hk, d)
    vc = v.astype(jnp.float32).reshape(n, c, hk, d)
    dc = doc.reshape(n, c)
    pc = jnp.arange(seq).reshape(n, c)

    def per_query(jq):
        qd = dc[jq]
        qp = pc[jq]

        def step(carry, ik):
            kd = dc[ik]
            kp = pc[ik]

            def run(cr):
                m, l, acc = cr
                mask = (qd[:, None] == kd[None, :]) & (kp[None, :] <= qp[:, None])
                s = jnp.einsum('qhgd,khd->hgqk', qc[jq], kc[ik]) * scale
                s = jnp.where(mask, s, -1e30)
                m_new = jnp.maximum(m, jnp.max(s, axis=-1))
                p = jnp.where(mask, jnp.exp(s - m_new[..., None]), 0.0)
                corr = jnp.exp(m - m_new)
                l_new = l * corr + jnp.sum(p, axis=-1)
                acc_new = acc * corr[..., None] + jnp.einsum('hgqk,khd->hgqd', p, vc[ik])
                return m_new, l_new, acc_new

            need = (ik == jq) | ((ik < jq) & (kd[c - 1] == qd[0]))
            return lax.cond(need, run, lambda cr: cr, carry), None

        init = (jnp.full((hk, g, c), -1e30, jnp.float32), jnp.zeros((hk, g, c), jnp.float32), jnp.zeros((hk, g, c, d), jnp.float32))
        (m, l, acc), _ = lax.scan(step, init, jnp.arange(n))
        o = jnp.transpose(acc / l[..., None], (2, 0, 1, 3)).reshape(c, hq, d)
        lse = jnp.transpose(m + jnp.log(l), (2, 0, 1)).reshape(c, hq)
        return o, lse

    o, lse = lax.map(per_query, jnp.arange(n))
    return o.reshape(seq, hq, d), lse.reshape(seq, hq)


def setup_inputs(seed: int = 0, part: int = 0) -> dict:
    kp = jax.random.fold_in(jax.random.key(seed), part)
    kq, kk, kv, kg = jax.random.split(kp, 4)
    cu = _draw_cu(jax.random.fold_in(jax.random.key(seed + 1), 7))
    q = jax.random.normal(kq, (SEQ, GQA, HEAD), jnp.float32).astype(jnp.bfloat16)
    k = jax.random.normal(kk, (SEQ, 1, HEAD), jnp.float32).astype(jnp.bfloat16)
    v = jax.random.normal(kv, (SEQ, 1, HEAD), jnp.float32).astype(jnp.bfloat16)
    dout = jax.random.normal(kg, (SEQ, GQA, HEAD), jnp.float32).astype(jnp.bfloat16)
    out, lse = _forward(q, k, v, _doc_ids(cu, SEQ))
    return {'q': q, 'k': k, 'v': v, 'out': out.astype(jnp.bfloat16), 'dout': dout, 'lse': lse, 'cu_seqlens': cu}


def _scores(qb, kb, vb, gb, lse_t, dlt_t, mask, scale):
    s = jnp.einsum('qhgd,khd->hgqk', qb, kb) * scale
    p = jnp.exp(jnp.where(mask, s - lse_t[..., None], -1e30))
    dp = jnp.einsum('qhgd,khd->hgqk', gb, vb)
    ds = p * (dp - dlt_t[..., None])
    return p.astype(jnp.bfloat16).astype(jnp.float32), ds.astype(jnp.bfloat16).astype(jnp.float32)


def reference(q, k, v, out, dout, lse, cu_seqlens):
    seq, hq, d = q.shape
    hk = k.shape[1]
    g = hq // hk
    c = TOKENS_DEV
    n = seq // c
    scale = d ** -0.5
    doc = _doc_ids(cu_seqlens, seq).reshape(n, c)
    pos = jnp.arange(seq).reshape(n, c)
    qc = q.astype(jnp.float32).reshape(n, c, hk, g, d)
    gc = dout.astype(jnp.float32).reshape(n, c, hk, g, d)
    kc = k.astype(jnp.float32).reshape(n, c, hk, d)
    vc = v.astype(jnp.float32).reshape(n, c, hk, d)
    lse_t = jnp.transpose(lse.reshape(n, c, hk, g), (0, 2, 3, 1))
    dlt = jnp.sum(dout.astype(jnp.float32) * out.astype(jnp.float32), axis=-1)
    dlt_t = jnp.transpose(dlt.reshape(n, c, hk, g), (0, 2, 3, 1))

    def outer(dq, ik):
        kb = kc[ik]
        vb = vc[ik]
        kd = doc[ik]
        kp = pos[ik]

        def inner(carry, jq):
            def run(cr):
                dk, dv, dqa = cr
                mask = (doc[jq][:, None] == kd[None, :]) & (kp[None, :] <= pos[jq][:, None])
                pb, dsb = _scores(qc[jq], kb, vb, gc[jq], lse_t[jq], dlt_t[jq], mask, scale)
                dv = dv + jnp.einsum('hgqk,qhgd->khd', pb, gc[jq])
                dk = dk + jnp.einsum('hgqk,qhgd->khd', dsb, qc[jq]) * scale
                dqa = dqa.at[jq].add(jnp.einsum('hgqk,khd->qhgd', dsb, kb) * scale)
                return dk, dv, dqa

            need = (jq == ik) | ((jq > ik) & (doc[jq][0] == kd[c - 1]))
            return lax.cond(need, run, lambda cr: cr, carry), None

        zero = jnp.zeros((c, hk, d), jnp.float32)
        (dk, dv, dq), _ = lax.scan(inner, (zero, zero, dq), jnp.arange(n))
        return dq, (dk, dv)

    dq, (dk, dv) = lax.scan(outer, jnp.zeros((n, c, hk, g, d), jnp.float32), jnp.arange(n))
    return (dq.reshape(seq, hq, d).astype(jnp.bfloat16), dk.reshape(seq, hk, d).astype(jnp.bfloat16), dv.reshape(seq, hk, d).astype(jnp.bfloat16))
```

```python
import functools

import jax
import jax.numpy as jnp
from jax import lax
from jax.experimental import pallas as pl
from jax.experimental.pallas import tpu as pltpu
from jax.sharding import PartitionSpec as P

LOG2E = 1.4426950408889634
B = 256
BF = jnp.bfloat16
F32 = jnp.float32
AXES = ('cpo', 'cp')


def _nt(a, b):
    return lax.dot_general(a, b, (((1,), (1,)), ((), ())), preferred_element_type=F32)


def _nn(a, b):
    return lax.dot_general(a, b, (((1,), (0,)), ((), ())), preferred_element_type=F32)


def _me():
    return lax.axis_index('cpo') * 4 + lax.axis_index('cp')


def _next_start(cu, t):
    e = cu[cu.shape[0] - 1]
    for i in range(cu.shape[0] - 2, -1, -1):
        e = jnp.where(cu[i] > t, cu[i], e)
    return e


def _starts(cu, base, n):
    pos = base + lax.broadcasted_iota(jnp.int32, (1, n), 1)
    s = jnp.zeros((1, n), jnp.int32)
    for i in range(1, cu.shape[0] - 1):
        s = jnp.where(pos >= cu[i], cu[i], s)
    return s


def _attend(own, nq, tab, cu, qbase, qd, st, kv, kt, qs, dq, dkv, nb):
    c, hd = qd.shape[2], qd.shape[3]
    scale2 = LOG2E * hd ** -0.5
    for s in range(nq):
        qs[s] = _starts(cu, qbase[s], c)
    rows = lax.broadcasted_iota(jnp.int32, (B, B), 0)
    cols = lax.broadcasted_iota(jnp.int32, (B, B), 1)

    def block(b, _):
        kbase = tab[b]
        end = _next_start(cu, kbase + B - 1)
        dkv[b] = jnp.zeros((2, B, hd), F32)
        kt[...] = kv[b, 0].T
        for s in range(nq):
            if own:
                lo = lax.div(kbase - qbase[s], B)
                ok = True
            else:
                lo = 0
                ok = kbase < qbase[s]
            hi = jnp.where(ok, jnp.clip(lax.div(end - qbase[s] + B - 1, B), 0, c // B), 0)

            def tile(qb, _, s=s):
                q0 = pl.multiple_of(qb * B, B)
                w = pl.ds(q0, B)
                k, v = kv[b, 0], kv[b, 1]
                mask = rows >= qs[s, :, w] - kbase
                if own:
                    mask = mask & (rows - cols <= qbase[s] + q0 - kbase)
                q4 = jnp.concatenate([qd[s, h, w, :] for h in range(4)], 0)
                g4 = jnp.concatenate([qd[s, 4 + h, w, :] for h in range(4)], 0)
                l4 = jnp.concatenate([st[s, h:h + 1, w] for h in range(4)], 1)
                d4 = jnp.concatenate([st[s, 4 + h:5 + h, w] for h in range(4)], 1)
                m4 = jnp.concatenate([mask] * 4, 1)
                x = jnp.where(m4, _nt(k, q4) * scale2 - l4, -1e30)
                p = jnp.exp2(x)
                ds = (p * (_nt(v, g4) - d4)).astype(BF)
                dkv[b, 0] += _nn(ds, q4)
                dkv[b, 1] += _nn(p.astype(BF), g4)
                r = _nn(kt[...], ds)
                for h in range(4):
                    dq[s, h, :, w] += r[:, h * B:(h + 1) * B]
                return 0

            lax.fori_loop(lo, hi, tile, 0)
        return 0

    lax.fori_loop(0, nb, block, 0)


def _own_kernel(cu, qd_h, st_h, kv_h, dq_h, dkv_h, qd, st, kv, kt, qs, dq, dkv, tab, sem):
    c = qd.shape[2]
    base = _me() * c
    cps = [pltpu.make_async_copy(qd_h, qd.at[0], sem.at[0]), pltpu.make_async_copy(st_h, st.at[0], sem.at[1])]
    for b in range(c // B):
        tab[b] = base + b * B
        for t in range(2):
            cps.append(pltpu.make_async_copy(kv_h.at[t, pl.ds(b * B, B), :], kv.at[b, t], sem.at[2 + 2 * b + t]))
    for x in cps:
        x.start()
    dq[...] = jnp.zeros(dq.shape, F32)
    for x in cps:
        x.wait()
    _attend(True, 1, tab, cu, [base], qd, st, kv, kt, qs, dq, dkv, c // B)
    outs = [pltpu.make_async_copy(dq.at[0], dq_h, sem.at[0])]
    for b in range(c // B):
        for t in range(2):
            outs.append(pltpu.make_async_copy(dkv.at[b, t], dkv_h.at[t, pl.ds(b * B, B), :], sem.at[2 + 2 * b + t]))
    for x in outs:
        x.start()
    for x in outs:
        x.wait()


def _far_kernel(first, slots, *refs):
    ns = len(slots)
    cu, qd0, qd1, st0, st1 = refs[:5]
    kvs = refs[5:5 + ns]
    n = 5 + ns
    if first:
        kv_own, kv_ic, dq0_in = refs[n:n + 3]
        n += 3
    else:
        dq0_in, dq1_in = refs[n:n + 2]
        n += 2
    dq0_out, dq1_out = refs[n:n + 2]
    outs = refs[n + 2:n + 2 + ns + (1 if first else 0)]
    n += 2 + len(outs)
    qd, st, kv, kt, qs, dq, dkv, tab, sem = refs[n:]
    c = qd.shape[2]
    me = _me()
    r = lax.rem(me, 2)
    chip = lax.div(me, 2)
    cps = []

    def cp(a, b):
        cps.append(pltpu.make_async_copy(a, b, sem.at[len(cps)]))

    cp(qd0, qd.at[0])
    cp(qd1, qd.at[1])
    cp(st0, st.at[0])
    cp(st1, st.at[1])
    cp(dq0_in, dq.at[0])
    if not first:
        cp(dq1_in, dq.at[1])
    b = 0
    where = []
    for (dist, same), ref in zip(slots, kvs):
        src = (chip ^ dist) * 2 + (r if same else 1 - r)
        for l in ((0, 2) if same else (1,)):
            tab[b] = src * c + l * B
            row = (l // 2 if same else 0) * B
            for t in range(2):
                cp(ref.at[t, pl.ds(row, B), :], kv.at[b, t])
            where.append((b, row))
            b += 1
    for x in cps:
        x.start()
    if first:
        dq[1] = jnp.zeros(dq.shape[1:], F32)
        base = lax.div(me, 2) * 2 * c

        @pl.when(r == 0)
        def _():
            tab[b] = base
            tab[b + 1] = base + 2 * B
            ics = [pltpu.make_async_copy(kv_own.at[t, pl.ds(2 * i * B, B), :], kv.at[b + i, t], sem.at[len(cps) + 2 * i + t])
                   for i in range(2) for t in range(2)]
            for x in ics:
                x.start()
            for x in ics:
                x.wait()

        @pl.when(r == 1)
        def _():
            tab[b] = base + B
            tab[b + 1] = base + 8 * c
            ics = [pltpu.make_async_copy(kv_ic.at[t], kv.at[b, t], sem.at[len(cps) + t]) for t in range(2)]
            for x in ics:
                x.start()
            for x in ics:
                x.wait()
            kv[b + 1] = kv[b]
        nb = b + 2
    else:
        nb = b
    for x in cps:
        x.wait()
    _attend(False, 2, tab, cu, [me * c, (me ^ 1) * c], qd, st, kv, kt, qs, dq, dkv, nb)
    cps.clear()
    cp(dq.at[0], dq0_out)
    cp(dq.at[1], dq1_out)
    i = 0
    for (dist, same), o in zip(slots, outs):
        for l in ((0, 2) if same else (1,)):
            bb, row = where[i]
            for t in range(2):
                cp(dkv.at[bb, t], o.at[t, pl.ds(row, B), :])
            i += 1
    if first:
        for j in range(2):
            for t in range(2):
                cp(dkv.at[b + j, t], outs[-1].at[t, pl.ds(j * B, B), :])
    for x in cps:
        x.start()
    for x in cps:
        x.wait()


def _any(n):
    return [pl.BlockSpec(memory_space=pl.ANY)] * n


SMEM = pl.BlockSpec(memory_space=pltpu.SMEM)


def _scratch(nq, nb, c, hd):
    return [pltpu.VMEM((nq, 8, c, hd), BF), pltpu.VMEM((nq, 8, c), F32), pltpu.VMEM((nb, 2, B, hd), BF),
            pltpu.VMEM((hd, B), BF), pltpu.VMEM((nq, 1, c), jnp.int32), pltpu.VMEM((nq, 4, hd, c), F32),
            pltpu.VMEM((nb, 2, B, hd), F32), pltpu.SMEM((nb,), jnp.int32), pltpu.SemaphoreType.DMA((40,))]


def _cost(tiles):
    return pl.CostEstimate(flops=tiles * 5 * 2 * 4 * B * B * 128, bytes_accessed=tiles * 500000, transcendentals=tiles * 4 * B * B)


def _own_call(cu, qd, st, kv):
    c, hd = qd.shape[1:]
    return pl.pallas_call(
        _own_kernel,
        out_shape=(jax.ShapeDtypeStruct((4, hd, c), F32), jax.ShapeDtypeStruct((2, c, hd), F32)),
        in_specs=[SMEM] + _any(3), out_specs=tuple(_any(2)),
        scratch_shapes=_scratch(1, 3, c, hd), cost_estimate=_cost(6),
        compiler_params=pltpu.CompilerParams(vmem_limit_bytes=48 * 2 ** 20))(cu, qd, st, kv)


def _far_call(first, slots, cu, qds, sts, kvs, extra):
    c, hd = qds[0].shape[1:]
    nb = sum(2 if s else 1 for _, s in slots) + (2 if first else 0)
    outs = [jax.ShapeDtypeStruct((4, hd, c), F32)] * 2
    outs += [jax.ShapeDtypeStruct((2, 2 * B if s else B, hd), F32) for _, s in slots]
    if first:
        outs.append(jax.ShapeDtypeStruct((2, 2 * B, hd), F32))
    ops = [cu, *qds, *sts, *kvs, *extra]
    return pl.pallas_call(
        functools.partial(_far_kernel, first, slots),
        out_shape=tuple(outs), in_specs=[SMEM] + _any(len(ops) - 1), out_specs=tuple(_any(len(outs))),
        scratch_shapes=_scratch(2, nb, c, hd), cost_estimate=_cost(12),
        compiler_params=pltpu.CompilerParams(vmem_limit_bytes=48 * 2 ** 20))(*ops)


PAIRS = {
    'ac': {1: (0, 2), 2: (0,), 3: (1,)},
    'bd': {1: (0, 2), 2: (1,), 3: (1,)},
    'all': {1: (0, 2), 2: (0, 1), 3: (0, 1)},
}


def solution(mesh):
    tok = P(AXES, 'hp', None)
    tok2 = P(AXES, 'hp')

    def body(q, k, v, out, dout, lse, cu):
        c, hq, hd = q.shape
        scale = hd ** -0.5
        r = lax.rem(lax.axis_index('cp'), 2)

        dl = jnp.sum(dout.astype(F32) * out.astype(F32), axis=-1)
        qd = jnp.concatenate([jnp.transpose(q, (1, 0, 2)), jnp.transpose(dout, (1, 0, 2))], 0)
        st = jnp.concatenate([lse.T * LOG2E, dl.T], 0)
        kv = jnp.concatenate([k.reshape(1, c, hd), v.reshape(1, c, hd)], 0)
        kvs = jnp.concatenate([kv[:, :B], kv[:, 2 * B:]], 1)
        kvc = kv[:, B:2 * B]

        def perm(x, pairs):
            return lax.ppermute(x, AXES, pairs)

        swap = [(i, i ^ 1) for i in range(8)]

        def branch(name, qd, st, kv, kvs, kvc):
            pairs = {}
            for dist, srcs in PAIRS[name].items():
                pairs[dist, True] = [(2 * a + i, 2 * (a ^ dist) + i) for a in srcs for i in range(2)]
                pairs[dist, False] = [(2 * a + i, 2 * (a ^ dist) + 1 - i) for a in srcs for i in range(2)]
            back = {key: [(b, a) for a, b in p] for key, p in pairs.items()}
            far_c = [(d, False) for d in (1, 2, 3)]
            far_s = [(d, True) for d in (1, 2, 3)]
            qd1 = perm(qd, swap)
            st1 = perm(st, swap)
            kv_ic = perm(kvc, [(2 * i, 2 * i + 1) for i in range(4)])
            in_c = [perm(kvc, pairs[s]) for s in far_c]
            in_s = [perm(kvs, pairs[s]) for s in far_s]
            dq0, dkv = _own_call(cu, qd, st, kv)
            res = _far_call(True, far_c, cu, (qd, qd1), (st, st1), in_c, (kv, kv_ic, dq0))
            dq0, dq1, part_c, ic = res[0], res[1], res[2:5], res[5]
            ret_c = [perm(x, back[s]) for x, s in zip(part_c, far_c)]
            ret_c.append(perm(ic[:, :B], [(2 * i + 1, 2 * i) for i in range(4)]))
            res = _far_call(False, far_s, cu, (qd, qd1), (st, st1), in_s, (dq0, dq1))
            dq0, dq1, part_s = res[0], res[1], res[2:5]
            ret_s = [perm(x, back[s]) for x, s in zip(part_s, far_s)]
            ret_s.append(jnp.where(r == 0, ic, 0.0))
            dqx = perm(dq1, swap)
            dc = sum(ret_c)
            ds = sum(ret_s)
            dkv = dkv + jnp.concatenate([ds[:, :B], dc, ds[:, B:]], 1)
            dq = jnp.transpose(dq0 + dqx, (2, 0, 1)) * scale
            return (dq.astype(BF), (dkv[0] * scale).astype(BF).reshape(c, 1, hd), dkv[1].astype(BF).reshape(c, 1, hd))

        def joins(t, u):
            return jnp.min(jnp.where(cu > t, cu, 8 * c)) > u

        ac = joins(2 * c - 1, 4 * c)
        bd = joins(4 * c - 1, 6 * c)
        which = jnp.where(~bd, 0, jnp.where(~ac, 1, 2)).astype(jnp.int32)
        return lax.switch(which, [functools.partial(branch, n) for n in ('ac', 'bd', 'all')], qd, st, kv, kvs, kvc)

    return jax.shard_map(body, mesh=mesh, in_specs=(tok, tok, tok, tok, tok, tok2, P()), out_specs=(tok, tok, tok), check_vma=False)
```

```python
import functools

import jax
import jax.numpy as jnp
from jax import lax
from jax.experimental import pallas as pl
from jax.experimental.pallas import tpu as pltpu
from jax.sharding import PartitionSpec as P

LOG2E = 1.4426950408889634
C = 768
B = 256
H = C // 2
HD = 128
BF = jnp.bfloat16
F32 = jnp.float32
AXES = ('cpo', 'cp')

LONG = ((3, 7), (2, 7), (0, 4), (0, 5), (1, 6))
PATTERNS = tuple(tuple(0 if j <= a else a if j <= b else b for j in range(8)) for a, b in LONG) + ((0,) * 8,)


def _nt(a, b):
    return lax.dot_general(a, b, (((1,), (1,)), ((), ())), preferred_element_type=F32)


def _nn(a, b):
    return lax.dot_general(a, b, (((1,), (0,)), ((), ())), preferred_element_type=F32)


def _pick(i, values):
    out = values[-1]
    for n in range(len(values) - 2, -1, -1):
        out = jnp.where(i == n, values[n], out)
    return out


def _starts(cu, base):
    pos = base + lax.broadcasted_iota(jnp.int32, (1, C), 1)
    s = jnp.zeros((1, C), jnp.int32)
    for i in range(1, cu.shape[0] - 1):
        s = jnp.where(pos >= cu[i], cu[i], s)
    return s


def _tile(k, v, kt, qd, st, mask, dk, dv, dq, s, w):
    q4 = jnp.concatenate([qd[s, h, w, :] for h in range(4)], 0)
    g4 = jnp.concatenate([qd[s, 4 + h, w, :] for h in range(4)], 0)
    l4 = jnp.concatenate([st[s, h:h + 1, w] for h in range(4)], 1)
    d4 = jnp.concatenate([st[s, 4 + h:5 + h, w] for h in range(4)], 1)
    m4 = jnp.concatenate([mask] * 4, 1)
    x = jnp.where(m4, _nt(k, q4) * (LOG2E * HD ** -0.5) - l4, -1e30)
    p = jnp.exp2(x)
    ds = (p * (_nt(v, g4) - d4)).astype(BF)
    dk[...] += _nn(ds, q4)
    dv[...] += _nn(p.astype(BF), g4)
    r = _nn(kt, ds)
    for h in range(4):
        dq[s, h, :, w] += r[:, h * B:(h + 1) * B]


def _kernel(first, cu, qd_h, st_h, kv, dq_o, dkv_o, qd, st, kvr, qs, kto, ktf, dq, dqx, own, part, ret,
            loc, kv_send, kv_recv, q_send, q_recv, r_send, r_recv, d_send, d_recv):
    me = lax.axis_index('cpo') * 4 + lax.axis_index('cp')
    chip = lax.div(me, 2)
    r = lax.rem(me, 2)
    mate = me + 1 - 2 * r
    lows = [first[2 * c] for c in range(4)]
    low = _pick(chip, lows)
    high = _pick(chip, [first[2 * c + 1] for c in range(4)])

    def place(d):
        return (0, lax.div(d, 4), lax.rem(d, 4))

    def remote(src, dst, ss, rs, dev):
        return pltpu.make_async_remote_copy(src_ref=src, dst_ref=dst, send_sem=ss, recv_sem=rs,
                                            device_id=place(dev), device_id_type=pl.DeviceIdType.MESH)

    loads = [pltpu.make_async_copy(qd_h, qd.at[r], loc.at[0]), pltpu.make_async_copy(st_h, st.at[r], loc.at[1])]
    for x in loads:
        x.start()

    barrier = pltpu.get_barrier_semaphore()
    for i in range(1, 8):
        pl.semaphore_signal(barrier, inc=1, device_id=place(lax.rem(me + i, 8)), device_id_type=pl.DeviceIdType.MESH)
    pl.semaphore_wait(barrier, 7)

    q_x = remote(qd_h, qd.at[r], q_send.at[0], q_recv.at[0], mate)
    s_x = remote(st_h, st.at[r], q_send.at[1], q_recv.at[1], mate)
    q_x.start()
    s_x.start()

    def keys(tc, par):
        return remote(kv.at[:, :, par], kvr.at[me], kv_send.at[tc, par], kv_recv.at[me], 2 * tc + par)

    own_half = pltpu.make_async_copy(kv.at[:, :, 0], kvr.at[me], loc.at[2])
    mate_half = remote(kv.at[:, :, 1], kvr.at[me], kv_send.at[0, 1], kv_recv.at[me], mate)

    @pl.when(r == 0)
    def _():
        own_half.start()
        mate_half.start()

    def sends(act):
        for tc in range(1, 4):
            @pl.when((chip < tc) & (me >= lows[tc]))
            def _(tc=tc):
                for par in range(2):
                    act(keys(tc, par))

    sends(lambda x: x.start())

    for s in range(2):
        qs[s] = _starts(cu, (2 * chip + s) * C)
    dq[...] = jnp.zeros(dq.shape, F32)
    own[...] = jnp.zeros(own.shape, F32)
    for x in loads:
        x.wait()

    rows = lax.broadcasted_iota(jnp.int32, (B, B), 0)
    cols = lax.broadcasted_iota(jnp.int32, (B, B), 1)

    def own_block(kb, _):
        k = kv[0, kb].reshape(B, HD)
        v = kv[1, kb].reshape(B, HD)
        kto[...] = k.T

        def own_tile(qb, _):
            q0 = pl.multiple_of(qb * B, B)
            w = pl.ds(q0, B)
            mask = (rows >= qs[r, :, w] - (me * C + kb * B)) & (rows - cols <= q0 - kb * B)
            _tile(kv[0, kb].reshape(B, HD), kv[1, kb].reshape(B, HD), kto[...], qd, st, mask, own.at[0, kb], own.at[1, kb], dq, r, w)
            return 0

        lax.fori_loop(kb, C // B, own_tile, 0)
        return 0

    lax.fori_loop(0, 1, own_block, 0)

    frow = lax.broadcasted_iota(jnp.int32, (H, B), 0)
    frow = frow + lax.div(frow, 128) * 128 + r * 128

    def back(p):
        return remote(part.at[p], ret.at[me], r_send.at[p], r_recv.at[me], p)

    q_x.wait_recv()
    s_x.wait_recv()
    units = 1 + 2 * chip - low

    def unit(u, _):
        p = 2 * chip - u

        @pl.when((u == 0) & (r == 0))
        def _():
            own_half.wait()

        @pl.when((u > 0) | (r == 1))
        def _():
            remote(kv.at[:, :, 0], kvr.at[p], kv_send.at[0, 0], kv_recv.at[p], mate).wait_recv()

        ktf[...] = kvr[p, 0].reshape(H, HD).T
        part[p] = jnp.zeros((2, H, HD), F32)

        def far_tile(qb, _):
            s = lax.div(qb, C // B)
            w = pl.ds(pl.multiple_of(lax.rem(qb, C // B) * B, B), B)
            mask = frow >= qs[s, :, w] - p * C
            _tile(kvr[p, 0].reshape(H, HD), kvr[p, 1].reshape(H, HD), ktf[...], qd, st, mask, part.at[p, 0], part.at[p, 1], dq, s, w)
            return 0

        lo = jnp.where(u == 0, C // B, 0)
        hi = jnp.where((u == 0) | (p >= high), 2 * (C // B), C // B)
        lax.fori_loop(lo, hi, far_tile, 0)

        @pl.when((u > 0) | (r == 1))
        def _():
            back(p).start()

        return 0

    lax.fori_loop(0, units, unit, 0)

    lax.fori_loop(1, C // B, own_block, 0)

    d_x = remote(dq.at[1 - r], dqx, d_send, d_recv, mate)
    d_x.start()

    def add(p_from):
        par = lax.rem(p_from, 2)
        for t in range(2):
            for i in range(3):
                a = pl.ds(pl.multiple_of(par * 128, 128), 128)
                own[t, i, a, :] += ret[p_from, t, pl.ds(i * 128, 128), :]

    @pl.when(r == 0)
    def _():
        for t in range(2):
            for i in range(3):
                own[t, i, pl.ds(0, 128), :] += part[me, t, pl.ds(i * 128, 128), :]
        remote(part.at[0], ret.at[mate], r_send.at[0], r_recv.at[mate], mate).wait_recv()
        add(mate)

    def collect(d, _):
        @pl.when(me >= _pick(lax.div(d, 2), lows))
        def _():
            remote(part.at[0], ret.at[d], r_send.at[0], r_recv.at[d], mate).wait_recv()
            add(d)
        return 0

    lax.fori_loop(2 * chip + 2, 8, collect, 0)

    scale = HD ** -0.5
    for t in range(2):
        dkv_o[t] = (own[t] * (scale if t == 0 else 1.0)).astype(BF)

    d_x.wait_recv()

    def finish(h, _):
        dq_o[h] = ((dq[r, h] + dqx[h]) * scale).T.astype(BF)
        return 0

    lax.fori_loop(0, 4, finish, 0)

    q_x.wait_send()
    s_x.wait_send()
    d_x.wait_send()

    @pl.when(r == 0)
    def _():
        mate_half.wait_send()

    sends(lambda x: x.wait_send())

    def drain(u, _):
        @pl.when((u > 0) | (r == 1))
        def _():
            back(2 * chip - u).wait_send()
        return 0

    lax.fori_loop(0, units, drain, 0)


def _call(n, cu, qd, st, kv):
    vm = pl.BlockSpec(memory_space=pltpu.VMEM)
    hbm = pl.BlockSpec(memory_space=pl.ANY)
    dma = pltpu.SemaphoreType.DMA
    return pl.pallas_call(
        functools.partial(_kernel, PATTERNS[n]),
        out_shape=(jax.ShapeDtypeStruct((4, C, HD), BF), jax.ShapeDtypeStruct((2, 3, B, HD), BF)),
        in_specs=[pl.BlockSpec(memory_space=pltpu.SMEM), hbm, hbm, vm], out_specs=(vm, vm),
        scratch_shapes=[
            pltpu.VMEM((2, 8, C, HD), BF), pltpu.VMEM((2, 8, C), F32), pltpu.VMEM((8, 2, 3, 128, HD), BF),
            pltpu.VMEM((2, 1, C), jnp.int32), pltpu.VMEM((HD, B), BF), pltpu.VMEM((HD, H), BF),
            pltpu.VMEM((2, 4, HD, C), F32), pltpu.VMEM((4, HD, C), F32), pltpu.VMEM((2, 3, B, HD), F32),
            pltpu.VMEM((8, 2, H, HD), F32), pltpu.VMEM((8, 2, H, HD), F32),
            dma((3,)), dma((4, 2)), dma((8,)), dma((2,)), dma((2,)), dma((8,)), dma((8,)), dma, dma],
        compiler_params=pltpu.CompilerParams(vmem_limit_bytes=60 * 2 ** 20, collective_id=n, has_side_effects=True),
        name='fused%d' % n)(cu, qd, st, kv)


def solution(mesh):
    tok = P(AXES, 'hp', None)
    tok2 = P(AXES, 'hp')

    def body(q, k, v, out, dout, lse, cu):
        dl = jnp.sum(dout.astype(F32) * out.astype(F32), axis=-1)
        qd = jnp.concatenate([jnp.transpose(q, (1, 0, 2)), jnp.transpose(dout, (1, 0, 2))], 0)
        st = jnp.concatenate([lse.T * LOG2E, dl.T], 0)
        kv = jnp.stack([k.reshape(3, 2, 128, HD), v.reshape(3, 2, 128, HD)])
        at = jnp.arange(8) * C
        start = jnp.max(jnp.where(cu[None, :] <= at[:, None], cu[None, :], 0), axis=1)
        fits = jnp.all((start // C)[None, :] >= jnp.array(PATTERNS), axis=1)
        which = jnp.argmax(fits).astype(jnp.int32)
        dq, dkv = lax.switch(which, [functools.partial(_call, n) for n in range(len(PATTERNS))], cu, qd, st, kv)
        return jnp.transpose(dq, (1, 0, 2)), dkv[0].reshape(C, 1, HD), dkv[1].reshape(C, 1, HD)

    return jax.shard_map(body, mesh=mesh, in_specs=(tok, tok, tok, tok, tok, tok2, P()), out_specs=(tok, tok, tok), check_vma=False)
```

```python
import functools

import jax
import jax.numpy as jnp
from jax import lax
from jax.experimental import pallas as pl
from jax.experimental.pallas import tpu as pltpu
from jax.sharding import PartitionSpec as P

LOG2E = 1.4426950408889634
C = 768
B = 256
H = C // 2
HD = 128
BF = jnp.bfloat16
F32 = jnp.float32
AXES = ('cpo', 'cp')

LONG = ((3, 7), (2, 7), (0, 4), (0, 5), (1, 6))
PATTERNS = tuple(tuple(0 if j <= a else a if j <= b else b for j in range(8)) for a, b in LONG) + ((0,) * 8,)
ORDER = ((), (1, 0), (1, 3, 0, 2), (3, 5, 1, 2, 4, 0))
KEY_RELAY = ((), (), (2, 3), (2, 3), (), ())
GRAD_RELAY = ((3,), (2, 3), (), (), (3,), (3,))


def _nt(a, b):
    return lax.dot_general(a, b, (((1,), (1,)), ((), ())), preferred_element_type=F32)


def _nn(a, b):
    return lax.dot_general(a, b, (((1,), (0,)), ((), ())), preferred_element_type=F32)


def _pick(i, values):
    out = values[-1]
    for n in range(len(values) - 2, -1, -1):
        out = jnp.where(i == n, values[n], out)
    return out


def _starts(cu, base):
    pos = base + lax.broadcasted_iota(jnp.int32, (1, C), 1)
    s = jnp.zeros((1, C), jnp.int32)
    for i in range(1, cu.shape[0] - 1):
        s = jnp.where(pos >= cu[i], cu[i], s)
    return s


def _tile(k, v, kt, qd, st, mask, dk, dv, dq, s, w):
    q4 = jnp.concatenate([qd[s, h, w, :] for h in range(4)], 0)
    g4 = jnp.concatenate([qd[s, 4 + h, w, :] for h in range(4)], 0)
    l4 = jnp.concatenate([st[s, h:h + 1, w] for h in range(4)], 1)
    d4 = jnp.concatenate([st[s, 4 + h:5 + h, w] for h in range(4)], 1)
    m4 = jnp.concatenate([mask] * 4, 1)
    x = jnp.where(m4, _nt(k, q4) * (LOG2E * HD ** -0.5) - l4, -1e30)
    p = jnp.exp2(x)
    ds = (p * (_nt(v, g4) - d4)).astype(BF)
    dk[...] += _nn(ds, q4)
    dv[...] += _nn(p.astype(BF), g4)
    r = _nn(kt, ds)
    for h in range(4):
        dq[s, h, :, w] += r[:, h * B:(h + 1) * B]


def _kernel(first, key_relay, grad_relay, cu, qd_h, st_h, kv, dq_o, dkv_o, qd, st, kvr, qs, kto, ktf, dq, dqx, own, part, ret, kvx, gx,
            x_send, x_recv, loc, kv_send, kv_recv, q_send, q_recv, r_send, r_recv, d_send, d_recv):
    me = lax.axis_index('cpo') * 4 + lax.axis_index('cp')
    chip = lax.div(me, 2)
    r = lax.rem(me, 2)
    mate = me + 1 - 2 * r
    lows = [first[2 * c] for c in range(4)]
    lists = [(2 * c,) + tuple(p for p in ORDER[c] if p >= lows[c]) for c in range(4)]

    def source(u):
        return _pick(chip, [_pick(u, x) for x in lists])

    high = _pick(chip, [first[2 * c + 1] for c in range(4)])

    def place(d):
        return (0, lax.div(d, 4), lax.rem(d, 4))

    def remote(src, dst, ss, rs, dev):
        return pltpu.make_async_remote_copy(src_ref=src, dst_ref=dst, send_sem=ss, recv_sem=rs,
                                            device_id=place(dev), device_id_type=pl.DeviceIdType.MESH)

    loads = [pltpu.make_async_copy(qd_h, qd.at[r], loc.at[0]), pltpu.make_async_copy(st_h, st.at[r], loc.at[1])]
    for x in loads:
        x.start()

    barrier = pltpu.get_barrier_semaphore()
    for i in range(1, 8):
        pl.semaphore_signal(barrier, inc=1, device_id=place(lax.rem(me + i, 8)), device_id_type=pl.DeviceIdType.MESH)
    pl.semaphore_wait(barrier, 7)

    q_x = remote(qd_h, qd.at[r], q_send.at[0], q_recv.at[0], mate)
    s_x = remote(st_h, st.at[r], q_send.at[1], q_recv.at[1], mate)
    q_x.start()
    s_x.start()

    def keys(tc, par):
        return remote(kv.at[:, :, par], kvr.at[me], kv_send.at[tc, par], kv_recv.at[me], 2 * tc + par)

    own_half = pltpu.make_async_copy(kv.at[:, :, 0], kvr.at[me], loc.at[2])
    mate_half = remote(kv.at[:, :, 1], kvr.at[me], kv_send.at[0, 1], kv_recv.at[me], mate)

    @pl.when(r == 0)
    def _():
        own_half.start()
        mate_half.start()

    def sends(act):
        for tc in range(1, 4):
            @pl.when((chip < tc) & (me >= lows[tc]))
            def _(tc=tc):
                for par in range(2):
                    if tc == 2 and key_relay:
                        for p in key_relay:
                            @pl.when(me == p)
                            def _(p=p, par=par):
                                act(remote(kv.at[:, :, par], kvx.at[p - 2], kv_send.at[tc, par], x_recv.at[p - 2], 6 + par))

                        @pl.when(chip != 1)
                        def _(par=par):
                            act(keys(tc, par))
                    else:
                        act(keys(tc, par))

    sends(lambda x: x.start())

    for s in range(2):
        qs[s] = _starts(cu, (2 * chip + s) * C)
    dq[...] = jnp.zeros(dq.shape, F32)
    own[...] = jnp.zeros(own.shape, F32)
    for x in loads:
        x.wait()

    rows = lax.broadcasted_iota(jnp.int32, (B, B), 0)
    cols = lax.broadcasted_iota(jnp.int32, (B, B), 1)

    def own_block(kb, _):
        k = kv[0, kb].reshape(B, HD)
        v = kv[1, kb].reshape(B, HD)
        kto[...] = k.T

        def own_tile(qb, _):
            q0 = pl.multiple_of(qb * B, B)
            w = pl.ds(q0, B)
            mask = (rows >= qs[r, :, w] - (me * C + kb * B)) & (rows - cols <= q0 - kb * B)
            _tile(kv[0, kb].reshape(B, HD), kv[1, kb].reshape(B, HD), kto[...], qd, st, mask, own.at[0, kb], own.at[1, kb], dq, r, w)
            return 0

        lax.fori_loop(kb, C // B, own_tile, 0)
        return 0

    lax.fori_loop(0, 1, own_block, 0)

    frow = lax.broadcasted_iota(jnp.int32, (H, B), 0)
    frow = frow + lax.div(frow, 128) * 128 + r * 128

    def back(p, act):
        direct = remote(part.at[p], ret.at[me], r_send.at[p], r_recv.at[me], p)
        if not grad_relay:
            act(direct)
            return
        via = chip == 2
        via = via & ((p == 2) | (p == 3) if len(grad_relay) == 2 else p == grad_relay[0])

        @pl.when(via)
        def _():
            act(remote(part.at[p], gx.at[p - 2], r_send.at[p], x_recv.at[p - 2], r))

        @pl.when(jnp.logical_not(via))
        def _():
            act(direct)

    relay_k = [remote(kvx.at[p - 2], kvr.at[p], x_send.at[p - 2], kv_recv.at[p], 4 + r) for p in key_relay]
    relay_g = [remote(gx.at[p - 2], ret.at[4 + r], x_send.at[p - 2], r_recv.at[4 + r], p) for p in grad_relay]
    if key_relay:
        @pl.when(chip == 3)
        def _():
            for p, x in zip(key_relay, relay_k):
                remote(kvx.at[p - 2], kvx.at[p - 2], x_send.at[p - 2], x_recv.at[p - 2], mate).wait_recv()
                x.start()

    q_x.wait_recv()
    s_x.wait_recv()
    units = _pick(chip, [len(x) for x in lists])

    def unit(u, _):
        p = source(u)

        @pl.when((u == 0) & (r == 0))
        def _():
            own_half.wait()

        @pl.when((u > 0) | (r == 1))
        def _():
            remote(kv.at[:, :, 0], kvr.at[p], kv_send.at[0, 0], kv_recv.at[p], mate).wait_recv()

        ktf[...] = kvr[p, 0].reshape(H, HD).T
        part[p] = jnp.zeros((2, H, HD), F32)

        def far_tile(qb, _):
            s = lax.div(qb, C // B)
            w = pl.ds(pl.multiple_of(lax.rem(qb, C // B) * B, B), B)
            mask = frow >= qs[s, :, w] - p * C
            _tile(kvr[p, 0].reshape(H, HD), kvr[p, 1].reshape(H, HD), ktf[...], qd, st, mask, part.at[p, 0], part.at[p, 1], dq, s, w)
            return 0

        lo = jnp.where(u == 0, C // B, 0)
        hi = jnp.where((u == 0) | (p >= high), 2 * (C // B), C // B)
        lax.fori_loop(lo, hi, far_tile, 0)

        @pl.when((u > 0) | (r == 1))
        def _():
            back(p, lambda x: x.start())

        return 0

    lax.fori_loop(0, units, unit, 0)

    lax.fori_loop(1, C // B, own_block, 0)

    d_x = remote(dq.at[1 - r], dqx, d_send, d_recv, mate)
    d_x.start()

    if grad_relay:
        @pl.when(chip == 0)
        def _():
            for p, x in zip(reversed(grad_relay), reversed(relay_g)):
                remote(gx.at[p - 2], gx.at[p - 2], x_send.at[p - 2], x_recv.at[p - 2], mate).wait_recv()
                x.start()

    def add(p_from):
        par = lax.rem(p_from, 2)
        for t in range(2):
            for i in range(3):
                a = pl.ds(pl.multiple_of(par * 128, 128), 128)
                own[t, i, a, :] += ret[p_from, t, pl.ds(i * 128, 128), :]

    @pl.when(r == 0)
    def _():
        for t in range(2):
            for i in range(3):
                own[t, i, pl.ds(0, 128), :] += part[me, t, pl.ds(i * 128, 128), :]
        remote(part.at[0], ret.at[mate], r_send.at[0], r_recv.at[mate], mate).wait_recv()
        add(mate)

    def collect(d, _):
        @pl.when(me >= _pick(lax.div(d, 2), lows))
        def _():
            remote(part.at[0], ret.at[d], r_send.at[0], r_recv.at[d], mate).wait_recv()
            add(d)
        return 0

    lax.fori_loop(2 * chip + 2, 8, collect, 0)

    scale = HD ** -0.5
    for t in range(2):
        dkv_o[t] = (own[t] * (scale if t == 0 else 1.0)).astype(BF)

    d_x.wait_recv()

    def finish(h, _):
        dq_o[h] = ((dq[r, h] + dqx[h]) * scale).T.astype(BF)
        return 0

    lax.fori_loop(0, 4, finish, 0)

    q_x.wait_send()
    s_x.wait_send()
    d_x.wait_send()

    @pl.when(r == 0)
    def _():
        mate_half.wait_send()

    sends(lambda x: x.wait_send())
    for relays, where in ((relay_k, 3), (relay_g, 0)):
        if relays:
            @pl.when(chip == where)
            def _(relays=relays):
                for x in relays:
                    x.wait_send()

    def drain(u, _):
        @pl.when((u > 0) | (r == 1))
        def _():
            back(source(u), lambda x: x.wait_send())
        return 0

    lax.fori_loop(0, units, drain, 0)


def _call(n, cu, qd, st, kv):
    vm = pl.BlockSpec(memory_space=pltpu.VMEM)
    hbm = pl.BlockSpec(memory_space=pl.ANY)
    dma = pltpu.SemaphoreType.DMA
    return pl.pallas_call(
        functools.partial(_kernel, PATTERNS[n], KEY_RELAY[n], GRAD_RELAY[n]),
        out_shape=(jax.ShapeDtypeStruct((4, C, HD), BF), jax.ShapeDtypeStruct((2, 3, B, HD), BF)),
        in_specs=[pl.BlockSpec(memory_space=pltpu.SMEM), hbm, hbm, vm], out_specs=(vm, vm),
        scratch_shapes=[
            pltpu.VMEM((2, 8, C, HD), BF), pltpu.VMEM((2, 8, C), F32), pltpu.VMEM((8, 2, 3, 128, HD), BF),
            pltpu.VMEM((2, 1, C), jnp.int32), pltpu.VMEM((HD, B), BF), pltpu.VMEM((HD, H), BF),
            pltpu.VMEM((2, 4, HD, C), F32), pltpu.VMEM((4, HD, C), F32), pltpu.VMEM((2, 3, B, HD), F32),
            pltpu.VMEM((8, 2, H, HD), F32), pltpu.VMEM((8, 2, H, HD), F32),
            pltpu.VMEM((2, 2, 3, 128, HD), BF), pltpu.VMEM((2, 2, H, HD), F32),
            dma((2,)), dma((2,)), dma((3,)), dma((4, 2)), dma((8,)), dma((2,)), dma((2,)), dma((8,)), dma((8,)), dma, dma],
        compiler_params=pltpu.CompilerParams(vmem_limit_bytes=60 * 2 ** 20, collective_id=n, has_side_effects=True),
        name='fused%d' % n)(cu, qd, st, kv)


def solution(mesh):
    tok = P(AXES, 'hp', None)
    tok2 = P(AXES, 'hp')

    def body(q, k, v, out, dout, lse, cu):
        dl = jnp.sum(dout.astype(F32) * out.astype(F32), axis=-1)
        qd = jnp.concatenate([jnp.transpose(q, (1, 0, 2)), jnp.transpose(dout, (1, 0, 2))], 0)
        st = jnp.concatenate([lse.T * LOG2E, dl.T], 0)
        kv = jnp.stack([k.reshape(3, 2, 128, HD), v.reshape(3, 2, 128, HD)])
        at = jnp.arange(8) * C
        start = jnp.max(jnp.where(cu[None, :] <= at[:, None], cu[None, :], 0), axis=1)
        fits = jnp.all((start // C)[None, :] >= jnp.array(PATTERNS), axis=1)
        which = jnp.argmax(fits).astype(jnp.int32)
        dq, dkv = lax.switch(which, [functools.partial(_call, n) for n in range(len(PATTERNS))], cu, qd, st, kv)
        return jnp.transpose(dq, (1, 0, 2)), dkv[0].reshape(C, 1, HD), dkv[1].reshape(C, 1, HD)

    return jax.shard_map(body, mesh=mesh, in_specs=(tok, tok, tok, tok, tok, tok2, P()), out_specs=(tok, tok, tok), check_vma=False)
```

```python
import functools

import jax
import jax.numpy as jnp
from jax import lax
from jax.experimental import pallas as pl
from jax.experimental.pallas import tpu as pltpu
from jax.sharding import PartitionSpec as P

LOG2E = 1.4426950408889634
C = 768
B = 256
H = C // 2
HD = 128
BF = jnp.bfloat16
F32 = jnp.float32
AXES = ('cpo', 'cp')

LONG = ((3, 15), (2, 15), (0, 8), (0, 9), (0, 10), (0, 11), (1, 13), (1, 15))
PATTERNS = tuple(tuple(0 if j // 2 <= a else a if j <= b else b // 2 for j in range(16)) for a, b in LONG) + ((0,) * 16,)
ORDER = ((), (1, 0), (1, 3, 0, 2), (3, 5, 1, 2, 4, 0))
KEY_RELAY = ((), ()) + ((3, 2),) * 4 + ((),) * 3
GRAD_RELAY = ((3,), (3, 2)) + ((),) * 4 + ((3,),) * 3


def _nt(a, b):
    return lax.dot_general(a, b, (((1,), (1,)), ((), ())), preferred_element_type=F32)


def _nn(a, b):
    return lax.dot_general(a, b, (((1,), (0,)), ((), ())), preferred_element_type=F32)


def _pick(i, values):
    out = values[-1]
    for n in range(len(values) - 2, -1, -1):
        out = jnp.where(i == n, values[n], out)
    return out


def _starts(cu, base):
    pos = base + lax.broadcasted_iota(jnp.int32, (1, C), 1)
    s = jnp.zeros((1, C), jnp.int32)
    for i in range(1, cu.shape[0] - 1):
        s = jnp.where(pos >= cu[i], cu[i], s)
    return s


def _tile(k, v, kt, qd, st, mask, dk, dv, dq, s, w, n):
    q4 = jnp.concatenate([qd[s, h, w, :] for h in range(4)], 0)
    g4 = jnp.concatenate([qd[s, 4 + h, w, :] for h in range(4)], 0)
    l4 = jnp.concatenate([st[s, h:h + 1, w] for h in range(4)], 1)
    d4 = jnp.concatenate([st[s, 4 + h:5 + h, w] for h in range(4)], 1)
    m4 = jnp.concatenate([mask] * 4, 1)
    x = jnp.where(m4, _nt(k, q4) * (LOG2E * HD ** -0.5) - l4, -1e30)
    p = jnp.exp2(x)
    ds = (p * (_nt(v, g4) - d4)).astype(BF)
    dk[...] += _nn(ds, q4)
    dv[...] += _nn(p.astype(BF), g4)
    r = _nn(kt, ds)
    for h in range(4):
        dq[s, h, :, w] += r[:, h * n:(h + 1) * n]


def _kernel(first, key_relay, grad_relay, cu, qd_h, out_h, lse_h, k_h, v_h, dq_o, dk_o, dv_o, qd, st, kvr, qs, kto, ktf, dq, dqx,
            own, part, ret, kvx, gx, x_send, x_recv, loc, kv_send, kv_recv, q_send, q_recv, r_send, r_recv, d_send, d_recv):
    me = lax.axis_index('cpo') * 4 + lax.axis_index('cp')
    chip = lax.div(me, 2)
    r = lax.rem(me, 2)
    mate = me + 1 - 2 * r
    kv_h = (k_h, v_h)
    lows = [first[4 * c] for c in range(4)]
    lists = [(2 * c,) + tuple(p for p in ORDER[c] if p >= lows[c]) for c in range(4)]
    units = _pick(chip, [len(x) for x in lists])

    def source(u):
        return _pick(chip, [_pick(u, x) for x in lists])

    def place(d):
        return (0, lax.div(d, 4), lax.rem(d, 4))

    def remote(src, dst, ss, rs, dev):
        return pltpu.make_async_remote_copy(src_ref=src, dst_ref=dst, send_sem=ss, recv_sem=rs,
                                            device_id=place(dev), device_id_type=pl.DeviceIdType.MESH)

    load = pltpu.make_async_copy(qd_h, qd.at[r], loc.at[0])
    load.start()

    barrier = pltpu.get_barrier_semaphore()
    for i in range(1, 8):
        pl.semaphore_signal(barrier, inc=1, device_id=place(lax.rem(me + i, 8)), device_id_type=pl.DeviceIdType.MESH)
    pl.semaphore_wait(barrier, 7)

    q_x = remote(qd_h, qd.at[r], q_send.at[0], q_recv.at[0], mate)
    s_x = remote(st.at[r], st.at[r], q_send.at[1], q_recv.at[1], mate)
    d_x = remote(dq.at[1 - r], dqx, d_send, d_recv, mate)

    own_half = [pltpu.make_async_copy(kv_h[t].at[:, 0], kvr.at[me, t], loc.at[1 + t]) for t in range(2)]
    mate_half = [remote(kv_h[t].at[:, 1], kvr.at[me, t], kv_send.at[0, 1, t], kv_recv.at[me, t], mate) for t in range(2)]

    def keys(tc, par, act):
        for t in range(2):
            act(remote(kv_h[t].at[:, par], kvr.at[me, t], kv_send.at[tc, par, t], kv_recv.at[me, t], 2 * tc + par))

    def keys_via(p, par, act):
        for t in range(2):
            act(remote(kv_h[t].at[:, par], kvx.at[p - 2, t], kv_send.at[2, par, t], x_recv.at[p - 2, t], 6 + par))

    def sends(act):
        for tc in range(1, 4):
            @pl.when((chip < tc) & (me >= lows[tc]))
            def _(tc=tc):
                for par in range(2):
                    if tc == 2 and key_relay:
                        for p in key_relay:
                            @pl.when(me == p)
                            def _(p=p, par=par):
                                keys_via(p, par, act)

                        @pl.when(chip != 1)
                        def _(par=par):
                            keys(tc, par, act)
                    else:
                        keys(tc, par, act)

    @pl.when(r == 1)
    def _():
        sends(lambda x: x.start())

    q_x.start()

    @pl.when(r == 0)
    def _():
        for x in own_half + mate_half:
            x.start()

    for s in range(2):
        qs[s] = _starts(cu, (2 * chip + s) * C)
    st[r, 0:4] = lse_h[...] * LOG2E
    load.wait()
    ones = jnp.ones((8, HD), BF)

    def prepare(h, _):
        x = qd[r, 4 + h].astype(F32) * out_h[h].astype(F32)
        hi = x.astype(BF)
        lo = (x - hi.astype(F32)).astype(BF)
        st[r, pl.ds(4 + h, 1)] = (_nt(ones, hi) + _nt(ones, lo))[0:1]
        for s in range(2):
            dq[s, h] = jnp.zeros((HD, C), F32)
        return 0

    lax.fori_loop(0, 4, prepare, 0)
    own[...] = jnp.zeros(own.shape, F32)

    rows = lax.broadcasted_iota(jnp.int32, (B, B), 0)
    cols = lax.broadcasted_iota(jnp.int32, (B, B), 1)
    frow = lax.broadcasted_iota(jnp.int32, (H, H), 0)
    frow = frow + lax.div(frow, 128) * 128 + r * 128

    def own_block(kb, _):
        kto[...] = k_h[kb].reshape(B, HD).T

        @pl.when(kb == 2)
        def _():
            d_x.start()

        def own_tile(qb, _):
            @pl.when((kb == 0) & (qb == 1))
            def _():
                s_x.start()

            q0 = pl.multiple_of(qb * B, B)
            w = pl.ds(q0, B)
            mask = (rows >= qs[r, :, w] - (me * C + kb * B)) & (rows - cols <= q0 - kb * B)
            _tile(k_h[kb].reshape(B, HD), v_h[kb].reshape(B, HD), kto[...], qd, st, mask, own.at[0, kb], own.at[1, kb], dq, r, w, B)
            return 0

        lax.fori_loop(kb, C // B, own_tile, 0)
        return 0

    relay_k = [remote(kvx.at[p - 2, t], kvr.at[p, t], x_send.at[p - 2, t], kv_recv.at[p, t], 4 + r) for p in key_relay for t in range(2)]
    relay_g = [remote(gx.at[p - 2], ret.at[4 + r], x_send.at[p - 2, 0], r_recv.at[4 + r], p) for p in grad_relay]

    def back(p, act):
        direct = remote(part.at[p], ret.at[me], r_send.at[p], r_recv.at[me], p)
        if not grad_relay:
            act(direct)
            return
        via = chip == 2
        via = via & ((p == 2) | (p == 3) if len(grad_relay) == 2 else p == grad_relay[0])

        @pl.when(via)
        def _():
            act(remote(part.at[p], gx.at[p - 2], r_send.at[p], x_recv.at[p - 2, 0], r))

        @pl.when(jnp.logical_not(via))
        def _():
            act(direct)

    def unit(u):
        p = source(u)

        @pl.when(u == 0)
        def _():
            @pl.when(r == 0)
            def _():
                sends(lambda x: x.start())

            if key_relay:
                @pl.when(chip == 3)
                def _():
                    for n, p in enumerate(key_relay):
                        for t in range(2):
                            remote(kvx.at[p - 2, t], kvx.at[p - 2, t], x_send.at[p - 2, t], x_recv.at[p - 2, t], mate).wait_recv()
                            relay_k[2 * n + t].start()
            q_x.wait_recv()
            s_x.wait_recv()

            @pl.when(r == 0)
            def _():
                for x in own_half:
                    x.wait()

        @pl.when((u > 0) | (r == 1))
        def _():
            for t in range(2):
                remote(kv_h[t].at[:, 0], kvr.at[p, t], kv_send.at[0, 0, t], kv_recv.at[p, t], mate).wait_recv()

        ktf[...] = kvr[p, 0].reshape(H, HD).T
        part[p] = jnp.zeros((2, H, HD), F32)

        def far_tile(qb, _):
            s = lax.div(qb, 2)
            w = pl.ds(pl.multiple_of(lax.rem(qb, 2) * H, 128), H)
            mask = frow >= qs[s, :, w] - p * C
            _tile(kvr[p, 0].reshape(H, HD), kvr[p, 1].reshape(H, HD), ktf[...], qd, st, mask, part.at[p, 0], part.at[p, 1], dq, s, w, H)
            return 0

        need = 1
        for i in range(1, 4):
            need = need + jnp.where(p >= _pick(chip, [first[4 * c + i] for c in range(4)]), 1, 0)
        lax.fori_loop(jnp.where(u == 0, 2, 0), jnp.where(u == 0, 4, need), far_tile, 0)

        @pl.when((u > 0) | (r == 1))
        def _():
            back(p, lambda x: x.start())

    def step(t, _):
        mine = (t == 0) | (t == units + 1)

        @pl.when(mine)
        def _():
            lax.fori_loop(jnp.where(t == 0, 0, 1), jnp.where(t == 0, 1, C // B), own_block, 0)

        @pl.when(jnp.logical_not(mine))
        def _():
            unit(t - 1)
        return 0

    lax.fori_loop(0, units + 2, step, 0)

    if grad_relay:
        @pl.when(chip == 0)
        def _():
            for p, x in zip(grad_relay, relay_g):
                remote(gx.at[p - 2], gx.at[p - 2], x_send.at[p - 2, 0], x_recv.at[p - 2, 0], mate).wait_recv()
                x.start()

    def add(src, d):
        a = pl.ds(pl.multiple_of(lax.rem(d, 2) * 128, 128), 128)
        for t in range(2):
            for i in range(3):
                own[t, i, a, :] += src[d, t, pl.ds(i * 128, 128), :]

    d_x.wait_recv()
    scale = HD ** -0.5

    def finish(h, _):
        dq_o[h] = ((dq[r, h] + dqx[h]) * scale).T.astype(BF)
        return 0

    lax.fori_loop(0, 4, finish, 0)

    @pl.when(r == 0)
    def _():
        add(part, me)
        remote(part.at[0], ret.at[mate], r_send.at[0], r_recv.at[mate], mate).wait_recv()
        add(ret, mate)

    def collect(d, _):
        @pl.when(me >= _pick(lax.div(d, 2), lows))
        def _():
            remote(part.at[0], ret.at[d], r_send.at[0], r_recv.at[d], mate).wait_recv()
            add(ret, d)
        return 0

    lax.fori_loop(2 * chip + 2, 8, collect, 0)
    dk_o[...] = (own[0].reshape(C, HD) * scale).astype(BF)
    dv_o[...] = own[1].reshape(C, HD).astype(BF)

    for x in (q_x, s_x, d_x):
        x.wait_send()

    @pl.when(r == 0)
    def _():
        for x in mate_half:
            x.wait_send()

    sends(lambda x: x.wait_send())
    for relays, where in ((relay_k, 3), (relay_g, 0)):
        if relays:
            @pl.when(chip == where)
            def _(relays=relays):
                for x in relays:
                    x.wait_send()

    def drain(u, _):
        @pl.when((u > 0) | (r == 1))
        def _():
            back(source(u), lambda x: x.wait_send())
        return 0

    lax.fori_loop(0, units, drain, 0)


def _call(n, cu, *ops):
    vm = pl.BlockSpec(memory_space=pltpu.VMEM)
    dma = pltpu.SemaphoreType.DMA
    return pl.pallas_call(
        functools.partial(_kernel, PATTERNS[n], KEY_RELAY[n], GRAD_RELAY[n]),
        out_shape=(jax.ShapeDtypeStruct((4, C, HD), BF), jax.ShapeDtypeStruct((C, HD), BF), jax.ShapeDtypeStruct((C, HD), BF)),
        in_specs=[pl.BlockSpec(memory_space=pltpu.SMEM), pl.BlockSpec(memory_space=pl.ANY)] + [vm] * 4, out_specs=(vm, vm, vm),
        scratch_shapes=[
            pltpu.VMEM((2, 8, C, HD), BF), pltpu.VMEM((2, 8, C), F32), pltpu.VMEM((8, 2, 3, 128, HD), BF),
            pltpu.VMEM((2, 1, C), jnp.int32), pltpu.VMEM((HD, B), BF), pltpu.VMEM((HD, H), BF),
            pltpu.VMEM((2, 4, HD, C), F32), pltpu.VMEM((4, HD, C), F32), pltpu.VMEM((2, 3, B, HD), F32),
            pltpu.VMEM((8, 2, H, HD), F32), pltpu.VMEM((8, 2, H, HD), F32),
            pltpu.VMEM((2, 2, 3, 128, HD), BF), pltpu.VMEM((2, 2, H, HD), F32),
            dma((2, 2)), dma((2, 2)), dma((3,)), dma((4, 2, 2)), dma((8, 2)), dma((2,)), dma((2,)), dma((8,)), dma((8,)), dma, dma],
        compiler_params=pltpu.CompilerParams(vmem_limit_bytes=52 * 2 ** 20, collective_id=n, has_side_effects=True),
        name='fused%d' % n)(cu, *ops)


def _which(cu):
    ok = None
    for j in range(1, 16):
        least = jnp.array([p[j] * C for p in PATTERNS], jnp.int32)
        if max(p[j] for p in PATTERNS) == 0:
            continue
        here = least == 0
        for i in range(1, cu.shape[0] - 1):
            here = here | ((cu[i] >= least) & (cu[i] <= j * H))
        ok = here if ok is None else ok & here
    return jnp.min(jnp.where(ok, jnp.arange(len(PATTERNS), dtype=jnp.int32), len(PATTERNS) - 1))


def solution(mesh):
    tok = P(AXES, 'hp', None)
    tok2 = P(AXES, 'hp')

    def body(q, k, v, out, dout, lse, cu):
        qd = jnp.concatenate([jnp.transpose(q, (1, 0, 2)), jnp.transpose(dout, (1, 0, 2))], 0)
        ops = (cu, qd, jnp.transpose(out, (1, 0, 2)), lse.T, k.reshape(3, 2, 128, HD), v.reshape(3, 2, 128, HD))
        dq, dk, dv = lax.switch(_which(cu), [functools.partial(_call, n) for n in range(len(PATTERNS))], *ops)
        return jnp.transpose(dq, (1, 0, 2)), dk.reshape(C, 1, HD), dv.reshape(C, 1, HD)

    return jax.shard_map(body, mesh=mesh, in_specs=(tok, tok, tok, tok, tok, tok2, P()), out_specs=(tok, tok, tok), check_vma=False)
```

```python
import functools

import jax
import jax.numpy as jnp
from jax import lax
from jax.experimental import pallas as pl
from jax.experimental.pallas import tpu as pltpu
from jax.sharding import PartitionSpec as P

LOG2E = 1.4426950408889634
C = 768
B = 256
H = C // 2
HD = 128
BF = jnp.bfloat16
F32 = jnp.float32
AXES = ('cpo', 'cp')

LONG = ((3, 15), (2, 15), (0, 8), (0, 9), (0, 10), (0, 11), (1, 13), (1, 15))
PATTERNS = tuple(tuple(0 if j // 2 <= a else a if j <= b else b // 2 for j in range(16)) for a, b in LONG) + ((0,) * 16,)
ORDER = ((), (1, 0), (1, 3, 0, 2), (3, 5, 1, 2, 4, 0))
KEY_RELAY = ((), ()) + ((3, 2),) * 4 + ((),) * 3
GRAD_RELAY = ((3,), (3, 2)) + ((),) * 4 + ((3,),) * 3


def _nt(a, b):
    return lax.dot_general(a, b, (((1,), (1,)), ((), ())), preferred_element_type=F32)


def _nn(a, b):
    return lax.dot_general(a, b, (((1,), (0,)), ((), ())), preferred_element_type=F32)


def _pick(i, values):
    out = values[-1]
    for n in range(len(values) - 2, -1, -1):
        out = jnp.where(i == n, values[n], out)
    return out


def _starts(cu, base):
    pos = base + lax.broadcasted_iota(jnp.int32, (1, C), 1)
    s = jnp.zeros((1, C), jnp.int32)
    for i in range(1, cu.shape[0] - 1):
        s = jnp.where(pos >= cu[i], cu[i], s)
    return s


def _tile(k, v, kt, qd, st, mask, dk, dv, dq, s, w, n):
    q4 = jnp.concatenate([qd[s, h, w, :] for h in range(4)], 0)
    g4 = jnp.concatenate([qd[s, 4 + h, w, :] for h in range(4)], 0)
    l4 = jnp.concatenate([st[s, h:h + 1, w] for h in range(4)], 1)
    d4 = jnp.concatenate([st[s, 4 + h:5 + h, w] for h in range(4)], 1)
    m4 = jnp.concatenate([mask] * 4, 1)
    x = jnp.where(m4, _nt(k, q4) * (LOG2E * HD ** -0.5) - l4, -1e30)
    p = jnp.exp2(x)
    ds = (p * (_nt(v, g4) - d4)).astype(BF)
    dk[...] += _nn(ds, q4)
    dv[...] += _nn(p.astype(BF), g4)
    r = _nn(kt, ds)
    for h in range(4):
        dq[s, h, :, w] += r[:, h * n:(h + 1) * n]


def _kernel(first, key_relay, grad_relay, cu, qd_h, out_h, lse_h, k_h, v_h, dq_o, dk_o, dv_o, qd, st, kvr, qs, kto, ktf, dq, dqx,
            own, part, ret, kvx, gx, x_send, x_recv, loc, kv_send, kv_recv, q_send, q_recv, r_send, r_recv, d_send, d_recv):
    me = lax.axis_index('cpo') * 4 + lax.axis_index('cp')
    chip = lax.div(me, 2)
    r = lax.rem(me, 2)
    mate = me + 1 - 2 * r
    kv_h = (k_h, v_h)
    lows = [first[4 * c] for c in range(4)]
    lists = [(2 * c,) + tuple(p for p in ORDER[c] if p >= lows[c]) for c in range(4)]
    units = _pick(chip, [len(x) for x in lists])

    def source(u):
        return _pick(chip, [_pick(u, x) for x in lists])

    def place(d):
        return (0, lax.div(d, 4), lax.rem(d, 4))

    def remote(src, dst, ss, rs, dev):
        return pltpu.make_async_remote_copy(src_ref=src, dst_ref=dst, send_sem=ss, recv_sem=rs,
                                            device_id=place(dev), device_id_type=pl.DeviceIdType.MESH)

    load = pltpu.make_async_copy(qd_h, qd.at[r], loc.at[0])
    load.start()

    barrier = pltpu.get_barrier_semaphore()
    for i in range(1, 8):
        pl.semaphore_signal(barrier, inc=1, device_id=place(lax.rem(me + i, 8)), device_id_type=pl.DeviceIdType.MESH)
    pl.semaphore_wait(barrier, 7)

    q_x = remote(qd_h, qd.at[r], q_send.at[0], q_recv.at[0], mate)
    s_x = remote(st.at[r], st.at[r], q_send.at[1], q_recv.at[1], mate)
    d_x = remote(dq.at[1 - r], dqx, d_send, d_recv, mate)

    own_half = [pltpu.make_async_copy(kv_h[t].at[:, 0], kvr.at[me, t], loc.at[1 + t]) for t in range(2)]
    mate_half = [remote(kv_h[t].at[:, 1], kvr.at[me, t], kv_send.at[0, 1, t], kv_recv.at[me, t], mate) for t in range(2)]

    def keys(tc, par, act):
        for t in range(2):
            act(remote(kv_h[t].at[:, par], kvr.at[me, t], kv_send.at[tc, par, t], kv_recv.at[me, t], 2 * tc + par))

    def keys_via(p, par, act):
        for t in range(2):
            act(remote(kv_h[t].at[:, par], kvx.at[p - 2, t], kv_send.at[2, par, t], x_recv.at[p - 2, t], 6 + par))

    def sends(act):
        for tc in range(1, 4):
            @pl.when((chip < tc) & (me >= lows[tc]))
            def _(tc=tc):
                for par in range(2):
                    if tc == 2 and key_relay:
                        for p in key_relay:
                            @pl.when(me == p)
                            def _(p=p, par=par):
                                keys_via(p, par, act)

                        @pl.when(chip != 1)
                        def _(par=par):
                            keys(tc, par, act)
                    else:
                        keys(tc, par, act)

    @pl.when(r == 1)
    def _():
        sends(lambda x: x.start())

    q_x.start()

    @pl.when(r == 0)
    def _():
        for x in own_half + mate_half:
            x.start()

    for s in range(2):
        qs[s] = _starts(cu, (2 * chip + s) * C)
    st[r, 0:4] = lse_h[...] * LOG2E
    load.wait()
    ones = jnp.ones((8, HD), BF)

    def prepare(h, _):
        x = qd[r, 4 + h].astype(F32) * out_h[h].astype(F32)
        hi = x.astype(BF)
        lo = (x - hi.astype(F32)).astype(BF)
        st[r, pl.ds(4 + h, 1)] = (_nt(ones, hi) + _nt(ones, lo))[0:1]
        for s in range(2):
            dq[s, h] = jnp.zeros((HD, C), F32)
        return 0

    lax.fori_loop(0, 4, prepare, 0)
    own[...] = jnp.zeros(own.shape, F32)

    rows = lax.broadcasted_iota(jnp.int32, (B, B), 0)
    cols = lax.broadcasted_iota(jnp.int32, (B, B), 1)
    frow = lax.broadcasted_iota(jnp.int32, (H, H), 0)
    frow = frow + lax.div(frow, 128) * 128 + r * 128

    def own_block(kb, _):
        kto[...] = k_h[kb].reshape(B, HD).T

        @pl.when(kb == 2)
        def _():
            d_x.start()

        def own_tile(qb, _):
            @pl.when((kb == 0) & (qb == 1))
            def _():
                s_x.start()

            q0 = pl.multiple_of(qb * B, B)
            w = pl.ds(q0, B)
            mask = (rows >= qs[r, :, w] - (me * C + kb * B)) & (rows - cols <= q0 - kb * B)
            _tile(k_h[kb].reshape(B, HD), v_h[kb].reshape(B, HD), kto[...], qd, st, mask, own.at[0, kb], own.at[1, kb], dq, r, w, B)
            return 0

        lax.fori_loop(kb, C // B, own_tile, 0)
        return 0

    relay_k = [remote(kvx.at[p - 2, t], kvr.at[p, t], x_send.at[p - 2, t], kv_recv.at[p, t], 4 + r) for p in key_relay for t in range(2)]
    relay_g = [remote(gx.at[p - 2], ret.at[4 + r], x_send.at[p - 2, 0], r_recv.at[4 + r], p) for p in grad_relay]

    def back(p, act):
        direct = remote(part.at[p], ret.at[me], r_send.at[p], r_recv.at[me], p)
        if not grad_relay:
            act(direct)
            return
        via = chip == 2
        via = via & ((p == 2) | (p == 3) if len(grad_relay) == 2 else p == grad_relay[0])

        @pl.when(via)
        def _():
            act(remote(part.at[p], gx.at[p - 2], r_send.at[p], x_recv.at[p - 2, 0], r))

        @pl.when(jnp.logical_not(via))
        def _():
            act(direct)

    def unit(u):
        p = source(u)

        @pl.when(u == 0)
        def _():
            @pl.when(r == 0)
            def _():
                sends(lambda x: x.start())

            if key_relay:
                @pl.when(chip == 3)
                def _():
                    for n, p in enumerate(key_relay):
                        for t in range(2):
                            remote(kvx.at[p - 2, t], kvx.at[p - 2, t], x_send.at[p - 2, t], x_recv.at[p - 2, t], mate).wait_recv()
                            relay_k[2 * n + t].start()
            q_x.wait_recv()
            s_x.wait_recv()

            @pl.when(r == 0)
            def _():
                for x in own_half:
                    x.wait()

        @pl.when((u > 0) | (r == 1))
        def _():
            for t in range(2):
                remote(kv_h[t].at[:, 0], kvr.at[p, t], kv_send.at[0, 0, t], kv_recv.at[p, t], mate).wait_recv()

        ktf[...] = kvr[p, 0].reshape(H, HD).T
        part[p] = jnp.zeros((2, H, HD), F32)

        def far_tile(qb, _):
            s = lax.div(qb, 2)
            w = pl.ds(pl.multiple_of(lax.rem(qb, 2) * H, 128), H)
            mask = frow >= qs[s, :, w] - p * C
            _tile(kvr[p, 0].reshape(H, HD), kvr[p, 1].reshape(H, HD), ktf[...], qd, st, mask, part.at[p, 0], part.at[p, 1], dq, s, w, H)
            return 0

        need = 1
        for i in range(1, 4):
            need = need + jnp.where(p >= _pick(chip, [first[4 * c + i] for c in range(4)]), 1, 0)
        lax.fori_loop(jnp.where(u == 0, 2, 0), jnp.where(u == 0, 4, need), far_tile, 0)

        @pl.when((u > 0) | (r == 1))
        def _():
            back(p, lambda x: x.start())

    def step(t, _):
        mine = (t == 0) | (t == units + 1)

        @pl.when(mine)
        def _():
            lax.fori_loop(jnp.where(t == 0, 0, 1), jnp.where(t == 0, 1, C // B), own_block, 0)

        @pl.when(jnp.logical_not(mine))
        def _():
            unit(t - 1)
        return 0

    lax.fori_loop(0, units + 2, step, 0)

    if grad_relay:
        @pl.when(chip == 0)
        def _():
            for p, x in zip(grad_relay, relay_g):
                remote(gx.at[p - 2], gx.at[p - 2], x_send.at[p - 2, 0], x_recv.at[p - 2, 0], mate).wait_recv()
                x.start()

    def add(src, d):
        a = pl.ds(pl.multiple_of(lax.rem(d, 2) * 128, 128), 128)
        for t in range(2):
            for i in range(3):
                own[t, i, a, :] += src[d, t, pl.ds(i * 128, 128), :]

    d_x.wait_recv()
    scale = HD ** -0.5

    def finish(h, _):
        dq_o[h] = ((dq[r, h] + dqx[h]) * scale).T.astype(BF)
        return 0

    lax.fori_loop(0, 4, finish, 0)

    @pl.when(r == 0)
    def _():
        add(part, me)
        remote(part.at[0], ret.at[mate], r_send.at[0], r_recv.at[mate], mate).wait_recv()
        add(ret, mate)

    def collect(d, _):
        @pl.when(me >= _pick(lax.div(d, 2), lows))
        def _():
            remote(part.at[0], ret.at[d], r_send.at[0], r_recv.at[d], mate).wait_recv()
            add(ret, d)
        return 0

    lax.fori_loop(2 * chip + 2, 8, collect, 0)
    dk_o[...] = (own[0].reshape(C, HD) * scale).astype(BF)
    dv_o[...] = own[1].reshape(C, HD).astype(BF)

    for x in (q_x, s_x, d_x):
        x.wait_send()

    @pl.when(r == 0)
    def _():
        for x in mate_half:
            x.wait_send()

    sends(lambda x: x.wait_send())
    for relays, where in ((relay_k, 3), (relay_g, 0)):
        if relays:
            @pl.when(chip == where)
            def _(relays=relays):
                for x in relays:
                    x.wait_send()

    def drain(u, _):
        @pl.when((u > 0) | (r == 1))
        def _():
            back(source(u), lambda x: x.wait_send())
        return 0

    lax.fori_loop(0, units, drain, 0)


def _call(n, cu, *ops):
    vm = pl.BlockSpec(memory_space=pltpu.VMEM)
    dma = pltpu.SemaphoreType.DMA
    return pl.pallas_call(
        functools.partial(_kernel, PATTERNS[n], KEY_RELAY[n], GRAD_RELAY[n]),
        out_shape=(jax.ShapeDtypeStruct((4, C, HD), BF), jax.ShapeDtypeStruct((C, HD), BF), jax.ShapeDtypeStruct((C, HD), BF)),
        in_specs=[pl.BlockSpec(memory_space=pltpu.SMEM), pl.BlockSpec(memory_space=pl.ANY)] + [vm] * 4, out_specs=(vm, vm, vm),
        scratch_shapes=[
            pltpu.VMEM((2, 8, C, HD), BF), pltpu.VMEM((2, 8, C), F32), pltpu.VMEM((8, 2, 3, 128, HD), BF),
            pltpu.VMEM((2, 1, C), jnp.int32), pltpu.VMEM((HD, B), BF), pltpu.VMEM((HD, H), BF),
            pltpu.VMEM((2, 4, HD, C), F32), pltpu.VMEM((4, HD, C), F32), pltpu.VMEM((2, 3, B, HD), F32),
            pltpu.VMEM((8, 2, H, HD), F32), pltpu.VMEM((8, 2, H, HD), F32),
            pltpu.VMEM((2, 2, 3, 128, HD), BF), pltpu.VMEM((2, 2, H, HD), F32),
            dma((2, 2)), dma((2, 2)), dma((3,)), dma((4, 2, 2)), dma((8, 2)), dma((2,)), dma((2,)), dma((8,)), dma((8,)), dma, dma],
        compiler_params=pltpu.CompilerParams(vmem_limit_bytes=52 * 2 ** 20, collective_id=n, has_side_effects=True),
        name='fused%d' % n)(cu, *ops)


def _which_kernel(cu, o):
    ok = [None] * len(PATTERNS)
    for j in range(1, 16):
        start = 0
        for i in range(1, cu.shape[0] - 1):
            start = jnp.where(cu[i] <= j * H, cu[i], start)
        for n, p in enumerate(PATTERNS):
            if p[j]:
                here = start >= p[j] * C
                ok[n] = here if ok[n] is None else ok[n] & here
    best = jnp.int32(len(PATTERNS) - 1)
    for n in range(len(PATTERNS) - 2, -1, -1):
        best = jnp.where(ok[n], n, best)
    o[0] = best


def _which(cu):
    smem = pl.BlockSpec(memory_space=pltpu.SMEM)
    return pl.pallas_call(_which_kernel, out_shape=jax.ShapeDtypeStruct((1,), jnp.int32),
                          in_specs=[smem], out_specs=smem, name='which')(cu)[0]


def solution(mesh):
    tok = P(AXES, 'hp', None)
    tok2 = P(AXES, 'hp')

    def body(q, k, v, out, dout, lse, cu):
        qd = jnp.concatenate([jnp.transpose(q, (1, 0, 2)), jnp.transpose(dout, (1, 0, 2))], 0)
        ops = (cu, qd, jnp.transpose(out, (1, 0, 2)), lse.T, k.reshape(3, 2, 128, HD), v.reshape(3, 2, 128, HD))
        dq, dk, dv = lax.switch(_which(cu), [functools.partial(_call, n) for n in range(len(PATTERNS))], *ops)
        return jnp.transpose(dq, (1, 0, 2)), dk.reshape(C, 1, HD), dv.reshape(C, 1, HD)

    return jax.shard_map(body, mesh=mesh, in_specs=(tok, tok, tok, tok, tok, tok2, P()), out_specs=(tok, tok, tok), check_vma=False)
```

```python
import functools

import jax
import jax.numpy as jnp
from jax import lax
from jax.experimental import pallas as pl
from jax.experimental.pallas import tpu as pltpu
from jax.sharding import PartitionSpec as P

LOG2E = 1.4426950408889634
C = 768
B = 256
H = C // 2
HD = 128
BF = jnp.bfloat16
F32 = jnp.float32
AXES = ('cpo', 'cp')

LONG = ((3, 15), (2, 15), (0, 8), (0, 9), (0, 10), (0, 11), (1, 13), (1, 15))
PATTERNS = tuple(tuple(0 if j // 2 <= a else a if j <= b else b // 2 for j in range(16)) for a, b in LONG) + ((0,) * 16,)
_LATE = ((3, 2, 1, 0), (2, 3, 1, 0), (5, 4, 1, 0, 3, 2), (5, 1, 0, 3, 2, 4))
_EARLY = ((1, 3, 0, 2), (1, 3, 2, 0), (5, 4), (5, 4))
_MIDDLE = ((3, 2, 1, 0), (3, 1, 2, 0), (5, 4, 1, 0, 3, 2), (5, 1, 0, 3, 2, 4))
ORDERS = (_LATE,) * 2 + (_EARLY,) * 4 + (_MIDDLE,) * 3
KEY_RELAY = ((), ()) + ((3, 2),) * 4 + ((),) * 3
GRAD_SUM = ((2,),) * 2 + ((),) * 4 + ((2, 3),) * 3
GRAD_RELAY = ((3,),) * 2 + ((),) * 7


def _nt(a, b):
    return lax.dot_general(a, b, (((1,), (1,)), ((), ())), preferred_element_type=F32)


def _nn(a, b):
    return lax.dot_general(a, b, (((1,), (0,)), ((), ())), preferred_element_type=F32)


def _pick(i, values):
    out = values[-1]
    for n in range(len(values) - 2, -1, -1):
        out = jnp.where(i == n, values[n], out)
    return out


def _starts(cu, base):
    pos = base + lax.broadcasted_iota(jnp.int32, (1, C), 1)
    s = jnp.zeros((1, C), jnp.int32)
    for i in range(1, cu.shape[0] - 1):
        s = jnp.where(pos >= cu[i], cu[i], s)
    return s


def _tile(k, v, kt, qd, st, mask, dk, dv, dq, s, w, n):
    q4 = jnp.concatenate([qd[s, h, w, :] for h in range(4)], 0)
    g4 = jnp.concatenate([qd[s, 4 + h, w, :] for h in range(4)], 0)
    l4 = jnp.concatenate([st[s, h:h + 1, w] for h in range(4)], 1)
    d4 = jnp.concatenate([st[s, 4 + h:5 + h, w] for h in range(4)], 1)
    m4 = jnp.concatenate([mask] * 4, 1)
    x = jnp.where(m4, _nt(k, q4) * (LOG2E * HD ** -0.5) - l4, -1e30)
    p = jnp.exp2(x)
    ds = (p * (_nt(v, g4) - d4)).astype(BF)
    dk[...] += _nn(ds, q4)
    dv[...] += _nn(p.astype(BF), g4)
    r = _nn(kt, ds)
    for h in range(4):
        dq[s, h, :, w] += r[:, h * n:(h + 1) * n]


def _kernel(first, orders, key_relay, grad_sum, grad_relay, cu, qd_h, out_h, lse_h, k_h, v_h, dq_o, own, qd, st, kvr, qs, kto, ktf, dq, dqx,
            part, ret, kvx, gx, x_send, x_recv, g_recv, loc, kv_send, kv_recv, q_send, q_recv, r_send, r_recv, d_send, d_recv):
    me = lax.axis_index('cpo') * 4 + lax.axis_index('cp')
    chip = lax.div(me, 2)
    r = lax.rem(me, 2)
    mate = me + 1 - 2 * r
    kv_h = (k_h, v_h)
    lows = [first[4 * c] for c in range(4)]
    order = ((), (), (1, 0), (1, 0)) + orders
    lists = [tuple(p for p in order[d] if p >= lows[d // 2]) + (d // 2 * 2,) for d in range(8)]
    units = _pick(chip, [len(lists[2 * c]) for c in range(4)])

    def source(u):
        return _pick(me, [_pick(u, x) for x in lists])

    def place(d):
        return (0, lax.div(d, 4), lax.rem(d, 4))

    def remote(src, dst, ss, rs, dev):
        return pltpu.make_async_remote_copy(src_ref=src, dst_ref=dst, send_sem=ss, recv_sem=rs,
                                            device_id=place(dev), device_id_type=pl.DeviceIdType.MESH)

    load = pltpu.make_async_copy(qd_h, qd.at[r], loc.at[0])
    load.start()

    barrier = pltpu.get_barrier_semaphore()
    for i in range(1, 8):
        pl.semaphore_signal(barrier, inc=1, device_id=place(lax.rem(me + i, 8)), device_id_type=pl.DeviceIdType.MESH)
    for s in range(2):
        qs[s] = _starts(cu, (2 * chip + s) * C)
    st[r, 0:4] = lse_h[...] * LOG2E
    ones = jnp.ones((8, HD), BF)

    def prepare(h, _):
        x = qd_h[4 + h].astype(F32) * out_h[h].astype(F32)
        hi = x.astype(BF)
        lo = (x - hi.astype(F32)).astype(BF)
        st[r, pl.ds(4 + h, 1)] = (_nt(ones, hi) + _nt(ones, lo))[0:1]
        for s in range(2):
            dq[s, h] = jnp.zeros((HD, C), F32)
        return 0

    lax.fori_loop(0, 4, prepare, 0)
    own[...] = jnp.zeros(own.shape, F32)

    pl.semaphore_wait(barrier, 7)

    q_x = remote(qd_h, qd.at[r], q_send.at[0], q_recv.at[0], mate)
    s_x = remote(st.at[r], st.at[r], q_send.at[1], q_recv.at[1], mate)
    d_x = remote(dq.at[1 - r], dqx, d_send, d_recv, mate)

    own_half = [pltpu.make_async_copy(kv_h[t].at[:, 0], kvr.at[me, t], loc.at[1 + t]) for t in range(2)]
    mate_half = [remote(kv_h[t].at[:, 1], kvr.at[me, t], kv_send.at[0, 1, t], kv_recv.at[me, t], mate) for t in range(2)]

    def keys(tc, par, act):
        for t in range(2):
            act(remote(kv_h[t].at[:, par], kvr.at[me, t], kv_send.at[tc, par, t], kv_recv.at[me, t], 2 * tc + par))

    def keys_via(p, par, act):
        for t in range(2):
            act(remote(kv_h[t].at[:, par], kvx.at[p - 2, t], kv_send.at[2, par, t], x_recv.at[p - 2, t], 6 + par))

    def sends(act):
        for tc in range(1, 4):
            @pl.when((chip < tc) & (me >= lows[tc]))
            def _(tc=tc):
                for par in range(2):
                    if tc == 2 and key_relay:
                        for p in key_relay:
                            @pl.when(me == p)
                            def _(p=p, par=par):
                                keys_via(p, par, act)

                        @pl.when(chip != 1)
                        def _(par=par):
                            keys(tc, par, act)
                    else:
                        keys(tc, par, act)

    @pl.when(r == 1)
    def _():
        sends(lambda x: x.start())

    q_x.start()

    @pl.when(r == 0)
    def _():
        for x in own_half + mate_half:
            x.start()

    load.wait()
    rows = lax.broadcasted_iota(jnp.int32, (B, B), 0)
    cols = lax.broadcasted_iota(jnp.int32, (B, B), 1)
    frow = lax.broadcasted_iota(jnp.int32, (H, H), 0)
    frow = frow + lax.div(frow, 128) * 128 + r * 128

    def own_block(kb, _):
        kto[...] = k_h[kb].reshape(B, HD).T

        @pl.when((kb == 1) & (r == 0))
        def _():
            sends(lambda x: x.start())

        def own_tile(qb, _):
            @pl.when((kb == 0) & (qb == 1))
            def _():
                s_x.start()

            q0 = pl.multiple_of(qb * B, B)
            w = pl.ds(q0, B)
            mask = (rows >= qs[r, :, w] - (me * C + kb * B)) & (rows - cols <= q0 - kb * B)
            _tile(k_h[kb].reshape(B, HD), v_h[kb].reshape(B, HD), kto[...], qd, st, mask, own.at[0, kb], own.at[1, kb], dq, r, w, B)
            return 0

        lax.fori_loop(kb, C // B, own_tile, 0)
        return 0

    relay_k = [remote(kvx.at[p - 2, t], kvr.at[p, t], x_send.at[p - 2, t], kv_recv.at[p, t], 4 + r) for p in key_relay for t in range(2)]

    def among(p, pieces):
        return functools.reduce(jnp.logical_or, [p == x for x in pieces])

    def back(p, act):
        rest = True
        for pieces, host in ((grad_sum, 6), (grad_relay, 0)):
            if pieces:
                via = (chip == 2) & among(p, pieces)
                rest = rest & jnp.logical_not(via)

                @pl.when(via)
                def _(host=host):
                    act(remote(part.at[p], gx.at[p - 2], r_send.at[p], g_recv.at[p - 2], host + r))

        @pl.when(rest)
        def _():
            act(remote(part.at[p], ret.at[me], r_send.at[p], r_recv.at[me], p))

    def unit(u):
        p = source(u)

        last = u == units - 1

        @pl.when(u == 0)
        def _():
            if key_relay:
                @pl.when(chip == 3)
                def _():
                    for n, p in enumerate(key_relay):
                        for t in range(2):
                            remote(kvx.at[p - 2, t], kvx.at[p - 2, t], x_send.at[p - 2, t], x_recv.at[p - 2, t], mate).wait_recv()
                            relay_k[2 * n + t].start()
            q_x.wait_recv()
            s_x.wait_recv()

        @pl.when(last & (r == 0))
        def _():
            for x in own_half:
                x.wait()

        @pl.when(jnp.logical_not(last) | (r == 1))
        def _():
            for t in range(2):
                remote(kv_h[t].at[:, 0], kvr.at[p, t], kv_send.at[0, 0, t], kv_recv.at[p, t], mate).wait_recv()

        ktf[...] = kvr[p, 0].reshape(H, HD).T
        part[p] = jnp.zeros((2, H, HD), F32)

        def far_tile(qb, _):
            s = lax.div(qb, 2)
            w = pl.ds(pl.multiple_of(lax.rem(qb, 2) * H, 128), H)
            mask = frow >= qs[s, :, w] - p * C
            _tile(kvr[p, 0].reshape(H, HD), kvr[p, 1].reshape(H, HD), ktf[...], qd, st, mask, part.at[p, 0], part.at[p, 1], dq, s, w, H)
            return 0

        need = 1
        for i in range(1, 4):
            need = need + jnp.where(p >= _pick(chip, [first[4 * c + i] for c in range(4)]), 1, 0)
        lax.fori_loop(jnp.where(last, 2, 0), jnp.where(last, 4, need), far_tile, 0)

        if grad_sum:
            @pl.when((chip == 3) & among(p, grad_sum))
            def _():
                remote(part.at[0], gx.at[p - 2], r_send.at[0], g_recv.at[p - 2], mate).wait_recv()
                part[p] += gx[p - 2]

        @pl.when(jnp.logical_not(last) | (r == 1))
        def _():
            back(p, lambda x: x.start())

    lax.fori_loop(0, C // B, own_block, 0)

    def step(u, _):
        @pl.when((u == units - 1) & (r == 1))
        def _():
            d_x.start()

        unit(u)
        return 0

    lax.fori_loop(0, units, step, 0)

    @pl.when(r == 0)
    def _():
        d_x.start()

    relay_g = [remote(gx.at[p - 2], ret.at[4 + r], x_send.at[p - 2, 0], r_recv.at[4 + r], p) for p in grad_relay]
    if grad_relay:
        @pl.when(chip == 0)
        def _():
            for p, x in zip(grad_relay, relay_g):
                remote(part.at[0], gx.at[p - 2], r_send.at[0], g_recv.at[p - 2], mate).wait_recv()
                x.start()

    def add(src, d):
        a = pl.ds(pl.multiple_of(lax.rem(d, 2) * 128, 128), 128)
        for t in range(2):
            for i in range(3):
                own[t, i, a, :] += src[d, t, pl.ds(i * 128, 128), :]

    d_x.wait_recv()
    scale = HD ** -0.5

    def finish(i, _):
        w = pl.ds(pl.multiple_of(i * 128, 128), 128)
        x = jnp.stack([((dq[r, h, :, w] + dqx[h, :, w]) * scale).T for h in range(4)], axis=0)
        dq_o[w] = jnp.transpose(x, (1, 0, 2)).astype(BF)
        return 0

    lax.fori_loop(0, C // 128, finish, 0)

    @pl.when(r == 0)
    def _():
        add(part, me)
        remote(part.at[0], ret.at[mate], r_send.at[0], r_recv.at[mate], mate).wait_recv()
        add(ret, mate)

    def collect(d, _):
        come = me >= _pick(lax.div(d, 2), lows)
        if grad_sum:
            come = come & jnp.logical_not(among(me, grad_sum) & ((d == 4) | (d == 5)))

        @pl.when(come)
        def _():
            remote(part.at[0], ret.at[d], r_send.at[0], r_recv.at[d], mate).wait_recv()
            add(ret, d)
        return 0

    lax.fori_loop(2 * chip + 2, 8, collect, 0)

    for x in (q_x, s_x, d_x):
        x.wait_send()

    @pl.when(r == 0)
    def _():
        for x in mate_half:
            x.wait_send()

    sends(lambda x: x.wait_send())
    for relays, host in ((relay_k, 3), (relay_g, 0)):
        if relays:
            @pl.when(chip == host)
            def _(relays=relays):
                for x in relays:
                    x.wait_send()

    def drain(u, _):
        @pl.when((u < units - 1) | (r == 1))
        def _():
            back(source(u), lambda x: x.wait_send())
        return 0

    lax.fori_loop(0, units, drain, 0)


def _call(n, cu, *ops):
    vm = pl.BlockSpec(memory_space=pltpu.VMEM)
    dma = pltpu.SemaphoreType.DMA
    return pl.pallas_call(
        functools.partial(_kernel, PATTERNS[n], ORDERS[n], KEY_RELAY[n], GRAD_SUM[n], GRAD_RELAY[n]),
        out_shape=(jax.ShapeDtypeStruct((C, 4, HD), BF), jax.ShapeDtypeStruct((2, 3, B, HD), F32)),
        in_specs=[pl.BlockSpec(memory_space=pltpu.SMEM)] + [vm] * 5, out_specs=(vm, vm),
        scratch_shapes=[
            pltpu.VMEM((2, 8, C, HD), BF), pltpu.VMEM((2, 8, C), F32), pltpu.VMEM((8, 2, 3, 128, HD), BF),
            pltpu.VMEM((2, 1, C), jnp.int32), pltpu.VMEM((HD, B), BF), pltpu.VMEM((HD, H), BF),
            pltpu.VMEM((2, 4, HD, C), F32), pltpu.VMEM((4, HD, C), F32),
            pltpu.VMEM((8, 2, H, HD), F32), pltpu.VMEM((8, 2, H, HD), F32),
            pltpu.VMEM((2, 2, 3, 128, HD), BF), pltpu.VMEM((2, 2, H, HD), F32),
            dma((2, 2)), dma((2, 2)), dma((2,)), dma((3,)), dma((4, 2, 2)), dma((8, 2)), dma((2,)), dma((2,)), dma((8,)), dma((8,)), dma, dma],
        compiler_params=pltpu.CompilerParams(vmem_limit_bytes=52 * 2 ** 20, collective_id=n, has_side_effects=True),
        name='fused%d' % n)(cu, *ops)


def _which_kernel(cu, o):
    ok = [None] * len(PATTERNS)
    for j in range(1, 16):
        start = 0
        for i in range(1, cu.shape[0] - 1):
            start = jnp.where(cu[i] <= j * H, cu[i], start)
        for n, p in enumerate(PATTERNS):
            if p[j]:
                here = start >= p[j] * C
                ok[n] = here if ok[n] is None else ok[n] & here
    best = jnp.int32(len(PATTERNS) - 1)
    for n in range(len(PATTERNS) - 2, -1, -1):
        best = jnp.where(ok[n], n, best)
    o[0] = best


def _which(cu):
    smem = pl.BlockSpec(memory_space=pltpu.SMEM)
    return pl.pallas_call(_which_kernel, out_shape=jax.ShapeDtypeStruct((1,), jnp.int32),
                          in_specs=[smem], out_specs=smem, name='which')(cu)[0]


def solution(mesh):
    tok = P(AXES, 'hp', None)
    tok2 = P(AXES, 'hp')

    def body(q, k, v, out, dout, lse, cu):
        qd = jnp.concatenate([jnp.transpose(q, (1, 0, 2)), jnp.transpose(dout, (1, 0, 2))], 0)
        ops = (cu, qd, jnp.transpose(out, (1, 0, 2)), lse.T, k.reshape(3, 2, 128, HD), v.reshape(3, 2, 128, HD))
        dq, dkv = lax.switch(_which(cu), [functools.partial(_call, n) for n in range(len(PATTERNS))], *ops)
        dkv = dkv.reshape(2, C, 1, HD)
        return dq, (dkv[0] * HD ** -0.5).astype(BF), dkv[1].astype(BF)

    return jax.shard_map(body, mesh=mesh, in_specs=(tok, tok, tok, tok, tok, tok2, P()), out_specs=(tok, tok, tok), check_vma=False)
```

```python
import functools

import jax
import jax.numpy as jnp
from jax import lax
from jax.experimental import pallas as pl
from jax.experimental.pallas import tpu as pltpu
from jax.sharding import PartitionSpec as P

LOG2E = 1.4426950408889634
C = 768
B = 256
H = C // 2
HD = 128
BF = jnp.bfloat16
F32 = jnp.float32
AXES = ('cpo', 'cp')

LONG = ((3, 15), (2, 15), (0, 8), (0, 9), (0, 10), (0, 11), (1, 13), (1, 15))
PATTERNS = tuple(tuple(0 if j // 2 <= a else a if j <= b else b // 2 for j in range(16)) for a, b in LONG) + ((0,) * 16,)
_LATE = ((3, 2, 1, 0), (2, 3, 1, 0), (5, 4, 1, 0, 3, 2), (5, 1, 0, 3, 2, 4))
_EARLY = ((1, 3, 2, 0), (1, 3, 0, 2), (5, 4), (5, 4))
_MIDDLE = ((3, 2, 1, 0), (3, 1, 2, 0), (5, 4, 1, 0, 3, 2), (5, 4, 1, 0, 3, 2))
ORDERS = (_LATE,) * 2 + (_EARLY,) * 4 + (_MIDDLE,) * 3
KEY_RELAY = ((), ()) + ((3, 2),) * 4 + ((),) * 3
GRAD_SUM = ((2,),) * 2 + ((),) * 4 + ((2, 3),) * 3
GRAD_RELAY = ((3,),) * 2 + ((),) * 7


def _nt(a, b):
    return lax.dot_general(a, b, (((1,), (1,)), ((), ())), preferred_element_type=F32)


def _nn(a, b):
    return lax.dot_general(a, b, (((1,), (0,)), ((), ())), preferred_element_type=F32)


def _pick(i, values):
    out = values[-1]
    for n in range(len(values) - 2, -1, -1):
        out = jnp.where(i == n, values[n], out)
    return out


def _starts(cu, base):
    pos = base + lax.broadcasted_iota(jnp.int32, (1, C), 1)
    s = jnp.zeros((1, C), jnp.int32)
    for i in range(1, cu.shape[0] - 1):
        s = jnp.where(pos >= cu[i], cu[i], s)
    return s


def _tile(k, v, kt, qd, st, mask, cut, dk, dv, dq, s, w, n):
    q4 = jnp.concatenate([qd[s, h, w, :] for h in range(4)], 0)
    g4 = jnp.concatenate([qd[s, 4 + h, w, :] for h in range(4)], 0)
    l4 = jnp.concatenate([st[s, h:h + 1, w] for h in range(4)], 1)
    d4 = jnp.concatenate([st[s, 4 + h:5 + h, w] for h in range(4)], 1)
    if cut is not None:
        l4 = jnp.where(jnp.concatenate([cut] * 4, 1), l4, 1e30)
    x = _nt(k, q4) * (LOG2E * HD ** -0.5) - l4
    if mask is not None:
        x = jnp.where(jnp.concatenate([mask] * 4, 1), x, -1e30)
    p = jnp.exp2(x)
    ds = (p * (_nt(v, g4) - d4)).astype(BF)
    dk[...] += _nn(ds, q4)
    dv[...] += _nn(p.astype(BF), g4)
    r = _nn(kt, ds)
    for h in range(4):
        dq[s, h, :, w] += r[:, h * n:(h + 1) * n]


def _kernel(first, orders, key_relay, grad_sum, grad_relay, cu, qd_h, out_h, lse_h, k_h, v_h, dq_o, own, qd, st, kvr, qs, kto, ktf, kf, dq, dqx,
            part, ret, kvx, gx, x_send, x_recv, g_recv, loc, kv_send, kv_recv, q_send, q_recv, r_send, r_recv, d_send, d_recv):
    me = lax.axis_index('cpo') * 4 + lax.axis_index('cp')
    chip = lax.div(me, 2)
    r = lax.rem(me, 2)
    mate = me + 1 - 2 * r
    kv_h = (k_h, v_h)
    lows = [first[4 * c] for c in range(4)]
    order = ((), (), (1, 0), (1, 0)) + orders
    lists = [tuple(p for p in order[d] if p >= lows[d // 2]) + (d // 2 * 2,) for d in range(8)]
    units = _pick(chip, [len(lists[2 * c]) for c in range(4)])

    def source(u):
        return _pick(me, [_pick(u, x) for x in lists])

    def place(d):
        return (0, lax.div(d, 4), lax.rem(d, 4))

    def remote(src, dst, ss, rs, dev):
        return pltpu.make_async_remote_copy(src_ref=src, dst_ref=dst, send_sem=ss, recv_sem=rs,
                                            device_id=place(dev), device_id_type=pl.DeviceIdType.MESH)

    load = pltpu.make_async_copy(qd_h, qd.at[r], loc.at[0])
    load.start()

    barrier = pltpu.get_barrier_semaphore()
    for i in range(1, 8):
        pl.semaphore_signal(barrier, inc=1, device_id=place(lax.rem(me + i, 8)), device_id_type=pl.DeviceIdType.MESH)
    for s in range(2):
        qs[s] = _starts(cu, (2 * chip + s) * C)
    st[r, 0:4] = lse_h[...] * LOG2E
    ones = jnp.ones((8, HD), BF)

    def prepare(h, _):
        x = qd_h[4 + h].astype(F32) * out_h[h].astype(F32)
        hi = x.astype(BF)
        lo = (x - hi.astype(F32)).astype(BF)
        st[r, pl.ds(4 + h, 1)] = (_nt(ones, hi) + _nt(ones, lo))[0:1]
        for s in range(2):
            dq[s, h] = jnp.zeros((HD, C), F32)
        return 0

    lax.fori_loop(0, 4, prepare, 0)
    own[...] = jnp.zeros(own.shape, F32)

    pl.semaphore_wait(barrier, 7)

    q_x = remote(qd_h, qd.at[r], q_send.at[0], q_recv.at[0], mate)
    s_x = remote(st.at[r], st.at[r], q_send.at[1], q_recv.at[1], mate)
    d_x = remote(dq.at[1 - r], dqx, d_send, d_recv, mate)

    own_half = [pltpu.make_async_copy(kv_h[t].at[:, 0], kvr.at[me, t], loc.at[1 + t]) for t in range(2)]
    mate_half = [remote(kv_h[t].at[:, 1], kvr.at[me, t], kv_send.at[0, 1, t], kv_recv.at[me, t], mate) for t in range(2)]

    def keys(tc, par, act):
        for t in range(2):
            act(remote(kv_h[t].at[:, par], kvr.at[me, t], kv_send.at[tc, par, t], kv_recv.at[me, t], 2 * tc + par))

    def keys_via(p, par, act):
        for t in range(2):
            act(remote(kv_h[t].at[:, par], kvx.at[p - 2, t], kv_send.at[2, par, t], x_recv.at[p - 2, t], 6 + par))

    def sends(act):
        for tc in range(1, 4):
            @pl.when((chip < tc) & (me >= lows[tc]))
            def _(tc=tc):
                for par in range(2):
                    if tc == 2 and key_relay:
                        for p in key_relay:
                            @pl.when(me == p)
                            def _(p=p, par=par):
                                keys_via(p, par, act)

                        @pl.when(chip != 1)
                        def _(par=par):
                            keys(tc, par, act)
                    else:
                        keys(tc, par, act)

    @pl.when(r == 1)
    def _():
        sends(lambda x: x.start())

    q_x.start()

    @pl.when(r == 0)
    def _():
        for x in own_half + mate_half:
            x.start()

    load.wait()
    rows = lax.broadcasted_iota(jnp.int32, (B, B), 0)
    cols = lax.broadcasted_iota(jnp.int32, (B, B), 1)
    frow = lax.broadcasted_iota(jnp.int32, (H, HD), 0)
    frow = frow + lax.div(frow, 128) * 128 + r * 128

    def own_block(kb, _):
        kto[...] = k_h[kb].reshape(B, HD).T

        @pl.when((kb == 1) & (r == 0))
        def _():
            sends(lambda x: x.start())

        def own_tile(qb, _):
            @pl.when((kb == 0) & (qb == 1))
            def _():
                s_x.start()

            q0 = pl.multiple_of(qb * B, B)
            w = pl.ds(q0, B)
            mask = (rows >= qs[r, :, w] - (me * C + kb * B)) & (rows - cols <= q0 - kb * B)
            _tile(k_h[kb].reshape(B, HD), v_h[kb].reshape(B, HD), kto[...], qd, st, mask, None, own.at[0, kb], own.at[1, kb], dq, r, w, B)
            return 0

        lax.fori_loop(kb, C // B, own_tile, 0)
        return 0

    relay_k = [remote(kvx.at[p - 2, t], kvr.at[p, t], x_send.at[p - 2, t], kv_recv.at[p, t], 4 + r) for p in key_relay for t in range(2)]

    def among(p, pieces):
        return functools.reduce(jnp.logical_or, [p == x for x in pieces])

    def back(p, act):
        rest = True
        for pieces, host in ((grad_sum, 6), (grad_relay, 0)):
            if pieces:
                via = (chip == 2) & among(p, pieces)
                rest = rest & jnp.logical_not(via)

                @pl.when(via)
                def _(host=host):
                    act(remote(part.at[p], gx.at[p - 2], r_send.at[p], g_recv.at[p - 2], host + r))

        @pl.when(rest)
        def _():
            act(remote(part.at[p], ret.at[me], r_send.at[p], r_recv.at[me], p))

    def unit(u):
        p = source(u)

        last = u == units - 1

        @pl.when(u == 0)
        def _():
            if key_relay:
                @pl.when(chip == 3)
                def _():
                    for n, p in enumerate(key_relay):
                        for t in range(2):
                            remote(kvx.at[p - 2, t], kvx.at[p - 2, t], x_send.at[p - 2, t], x_recv.at[p - 2, t], mate).wait_recv()
                            relay_k[2 * n + t].start()
            q_x.wait_recv()
            s_x.wait_recv()

        @pl.when(last & (r == 0))
        def _():
            for x in own_half:
                x.wait()

        @pl.when(jnp.logical_not(last) | (r == 1))
        def _():
            for t in range(2):
                remote(kv_h[t].at[:, 0], kvr.at[p, t], kv_send.at[0, 0, t], kv_recv.at[p, t], mate).wait_recv()

        end = p * C + C - 129 + r * 128
        since = 0
        for i in range(1, cu.shape[0] - 1):
            since = jnp.where(cu[i] <= end, cu[i], since)
        live = frow >= since - p * C
        k = kvr[p, 0].reshape(H, HD).astype(F32)
        kf[...] = jnp.where(live, k, k[H - 1:H]).astype(BF)
        ktf[...] = jnp.where(live, k, 0.0).astype(BF).T
        part[p] = jnp.zeros((2, H, HD), F32)

        def far_tile(qb, _):
            s = lax.div(qb, 2)
            w = pl.ds(pl.multiple_of(lax.rem(qb, 2) * H, 128), H)
            _tile(kf[...], kvr[p, 1].reshape(H, HD), ktf[...], qd, st, None, qs[s, :, w] <= end, part.at[p, 0], part.at[p, 1], dq, s, w, H)
            return 0

        need = 1
        for i in range(1, 4):
            need = need + jnp.where(p >= _pick(chip, [first[4 * c + i] for c in range(4)]), 1, 0)
        lax.fori_loop(jnp.where(last, 2, 0), jnp.where(last, 4, need), far_tile, 0)

        for t in range(2):
            part[p, t] = jnp.where(live, part[p, t], 0.0)

        if grad_sum:
            @pl.when((chip == 3) & among(p, grad_sum))
            def _():
                remote(part.at[0], gx.at[p - 2], r_send.at[0], g_recv.at[p - 2], mate).wait_recv()
                part[p] += gx[p - 2]

        @pl.when(jnp.logical_not(last) | (r == 1))
        def _():
            back(p, lambda x: x.start())

    lax.fori_loop(0, C // B, own_block, 0)

    def step(u, _):
        @pl.when((u == units - 1) & (r == 1))
        def _():
            d_x.start()

        unit(u)
        return 0

    lax.fori_loop(0, units, step, 0)

    @pl.when(r == 0)
    def _():
        d_x.start()

    relay_g = [remote(gx.at[p - 2], ret.at[4 + r], x_send.at[p - 2, 0], r_recv.at[4 + r], p) for p in grad_relay]
    if grad_relay:
        @pl.when(chip == 0)
        def _():
            for p, x in zip(grad_relay, relay_g):
                remote(part.at[0], gx.at[p - 2], r_send.at[0], g_recv.at[p - 2], mate).wait_recv()
                x.start()

    def add(src, d):
        a = pl.ds(pl.multiple_of(lax.rem(d, 2) * 128, 128), 128)
        for t in range(2):
            for i in range(3):
                own[t, i, a, :] += src[d, t, pl.ds(i * 128, 128), :]

    d_x.wait_recv()
    scale = HD ** -0.5

    def finish(i, _):
        w = pl.ds(pl.multiple_of(i * 128, 128), 128)
        x = jnp.stack([((dq[r, h, :, w] + dqx[h, :, w]) * scale).T for h in range(4)], axis=0)
        dq_o[w] = jnp.transpose(x, (1, 0, 2)).astype(BF)
        return 0

    lax.fori_loop(0, C // 128, finish, 0)

    @pl.when(r == 0)
    def _():
        add(part, me)
        remote(part.at[0], ret.at[mate], r_send.at[0], r_recv.at[mate], mate).wait_recv()
        add(ret, mate)

    def collect(d, _):
        come = me >= _pick(lax.div(d, 2), lows)
        if grad_sum:
            come = come & jnp.logical_not(among(me, grad_sum) & ((d == 4) | (d == 5)))

        @pl.when(come)
        def _():
            remote(part.at[0], ret.at[d], r_send.at[0], r_recv.at[d], mate).wait_recv()
            add(ret, d)
        return 0

    lax.fori_loop(2 * chip + 2, 8, collect, 0)

    for x in (q_x, s_x, d_x):
        x.wait_send()

    @pl.when(r == 0)
    def _():
        for x in mate_half:
            x.wait_send()

    sends(lambda x: x.wait_send())
    for relays, host in ((relay_k, 3), (relay_g, 0)):
        if relays:
            @pl.when(chip == host)
            def _(relays=relays):
                for x in relays:
                    x.wait_send()

    def drain(u, _):
        @pl.when((u < units - 1) | (r == 1))
        def _():
            back(source(u), lambda x: x.wait_send())
        return 0

    lax.fori_loop(0, units, drain, 0)


def _call(n, cu, *ops):
    vm = pl.BlockSpec(memory_space=pltpu.VMEM)
    dma = pltpu.SemaphoreType.DMA
    return pl.pallas_call(
        functools.partial(_kernel, PATTERNS[n], ORDERS[n], KEY_RELAY[n], GRAD_SUM[n], GRAD_RELAY[n]),
        out_shape=(jax.ShapeDtypeStruct((C, 4, HD), BF), jax.ShapeDtypeStruct((2, 3, B, HD), F32)),
        in_specs=[pl.BlockSpec(memory_space=pltpu.SMEM)] + [vm] * 5, out_specs=(vm, vm),
        scratch_shapes=[
            pltpu.VMEM((2, 8, C, HD), BF), pltpu.VMEM((2, 8, C), F32), pltpu.VMEM((8, 2, 3, 128, HD), BF),
            pltpu.VMEM((2, 1, C), jnp.int32), pltpu.VMEM((HD, B), BF), pltpu.VMEM((HD, H), BF), pltpu.VMEM((H, HD), BF),
            pltpu.VMEM((2, 4, HD, C), F32), pltpu.VMEM((4, HD, C), F32),
            pltpu.VMEM((8, 2, H, HD), F32), pltpu.VMEM((8, 2, H, HD), F32),
            pltpu.VMEM((2, 2, 3, 128, HD), BF), pltpu.VMEM((2, 2, H, HD), F32),
            dma((2, 2)), dma((2, 2)), dma((2,)), dma((3,)), dma((4, 2, 2)), dma((8, 2)), dma((2,)), dma((2,)), dma((8,)), dma((8,)), dma, dma],
        compiler_params=pltpu.CompilerParams(vmem_limit_bytes=52 * 2 ** 20, collective_id=n, has_side_effects=True),
        name='fused%d' % n)(cu, *ops)


def _which_kernel(cu, o):
    ok = [None] * len(PATTERNS)
    for j in range(1, 16):
        start = 0
        for i in range(1, cu.shape[0] - 1):
            start = jnp.where(cu[i] <= j * H, cu[i], start)
        for n, p in enumerate(PATTERNS):
            if p[j]:
                here = start >= p[j] * C
                ok[n] = here if ok[n] is None else ok[n] & here
    best = jnp.int32(len(PATTERNS) - 1)
    for n in range(len(PATTERNS) - 2, -1, -1):
        best = jnp.where(ok[n], n, best)
    o[0] = best


def _which(cu):
    smem = pl.BlockSpec(memory_space=pltpu.SMEM)
    return pl.pallas_call(_which_kernel, out_shape=jax.ShapeDtypeStruct((1,), jnp.int32),
                          in_specs=[smem], out_specs=smem, name='which')(cu)[0]


def solution(mesh):
    tok = P(AXES, 'hp', None)
    tok2 = P(AXES, 'hp')

    def body(q, k, v, out, dout, lse, cu):
        qd = jnp.concatenate([jnp.transpose(q, (1, 0, 2)), jnp.transpose(dout, (1, 0, 2))], 0)
        ops = (cu, qd, jnp.transpose(out, (1, 0, 2)), lse.T, k.reshape(3, 2, 128, HD), v.reshape(3, 2, 128, HD))
        dq, dkv = lax.switch(_which(cu), [functools.partial(_call, n) for n in range(len(PATTERNS))], *ops)
        dkv = dkv.reshape(2, C, 1, HD)
        return dq, (dkv[0] * HD ** -0.5).astype(BF), dkv[1].astype(BF)

    return jax.shard_map(body, mesh=mesh, in_specs=(tok, tok, tok, tok, tok, tok2, P()), out_specs=(tok, tok, tok), check_vma=False)
```

```python
import functools

import jax
import jax.numpy as jnp
from jax import lax
from jax.experimental import pallas as pl
from jax.experimental.pallas import tpu as pltpu
from jax.sharding import PartitionSpec as P

LOG2E = 1.4426950408889634
C = 768
B = 256
H = C // 2
HD = 128
BF = jnp.bfloat16
F32 = jnp.float32
AXES = ('cpo', 'cp')

LONG = ((3, 15), (2, 15), (0, 8), (0, 9), (0, 10), (0, 11), (1, 13), (1, 15))
PATTERNS = tuple(tuple(0 if j // 2 <= a else a if j <= b else b // 2 for j in range(16)) for a, b in LONG) + ((0,) * 16,)
_LATE = ((3, 2, 1, 0), (2, 3, 1, 0), (5, 4, 1, 0, 3, 2), (5, 1, 0, 3, 2, 4))
_CROSS = ((3, 2, 1, 0), (2, 3, 1, 0), (5, 3, 4, 2, 1, 0), (3, 5, 2, 4, 1, 0))
_EARLY = ((1, 3, 2, 0), (1, 3, 0, 2), (5, 4), (5, 4))
_MIDDLE = ((3, 2, 1, 0), (3, 1, 2, 0), (5, 4, 1, 0, 3, 2), (5, 4, 1, 0, 3, 2))
ORDERS = (_LATE, _CROSS) + (_EARLY,) * 4 + (_MIDDLE,) * 3
KEY_RELAY = ((), ()) + ((3, 2),) * 4 + ((),) * 3
GRAD_SUM = ((2,),) * 2 + ((),) * 4 + ((2, 3),) * 3
GRAD_RELAY = ((3,),) * 2 + ((),) * 7


def _nt(a, b):
    return lax.dot_general(a, b, (((1,), (1,)), ((), ())), preferred_element_type=F32)


def _nn(a, b):
    return lax.dot_general(a, b, (((1,), (0,)), ((), ())), preferred_element_type=F32)


def _pick(i, values):
    out = values[-1]
    for n in range(len(values) - 2, -1, -1):
        out = jnp.where(i == n, values[n], out)
    return out


def _starts(cu, base):
    pos = base + lax.broadcasted_iota(jnp.int32, (1, C), 1)
    s = jnp.zeros((1, C), jnp.int32)
    for i in range(1, cu.shape[0] - 1):
        s = jnp.where(pos >= cu[i], cu[i], s)
    return s


def _tile(k, v, kt, qd, st, mask, cut, dk, dv, dq, s, w, n):
    q4 = jnp.concatenate([qd[s, h, w, :] for h in range(4)], 0)
    g4 = jnp.concatenate([qd[s, 4 + h, w, :] for h in range(4)], 0)
    l4 = jnp.concatenate([st[s, h:h + 1, w] for h in range(4)], 1)
    d4 = jnp.concatenate([st[s, 4 + h:5 + h, w] for h in range(4)], 1)
    if cut is not None:
        l4 = jnp.where(jnp.concatenate([cut] * 4, 1), l4, 1e30)
    x = _nt(k, q4) * (LOG2E * HD ** -0.5) - l4
    if mask is not None:
        x = jnp.where(jnp.concatenate([mask] * 4, 1), x, -1e30)
    p = jnp.exp2(x)
    ds = (p * (_nt(v, g4) - d4)).astype(BF)
    dk[...] += _nn(ds, q4)
    dv[...] += _nn(p.astype(BF), g4)
    r = _nn(kt, ds)
    for h in range(4):
        dq[s, h, :, w] += r[:, h * n:(h + 1) * n]


def _kernel(first, orders, key_relay, grad_sum, grad_relay, cu, qd_h, out_h, lse_h, k_h, v_h, dq_o, own, qd, st, kvr, qs, kto, ktf, kf, dq, dqx,
            part, ret, kvx, gx, x_send, x_recv, g_recv, loc, kv_send, kv_recv, q_send, q_recv, r_send, r_recv, d_send, d_recv):
    me = lax.axis_index('cpo') * 4 + lax.axis_index('cp')
    chip = lax.div(me, 2)
    r = lax.rem(me, 2)
    mate = me + 1 - 2 * r
    kv_h = (k_h, v_h)
    lows = [first[4 * c] for c in range(4)]
    order = ((), (), (1, 0), (1, 0)) + orders
    lists = [tuple(p for p in order[d] if p >= lows[d // 2]) + (d // 2 * 2,) for d in range(8)]
    units = _pick(chip, [len(lists[2 * c]) for c in range(4)])

    def source(u):
        return _pick(me, [_pick(u, x) for x in lists])

    def place(d):
        return (0, lax.div(d, 4), lax.rem(d, 4))

    def remote(src, dst, ss, rs, dev):
        return pltpu.make_async_remote_copy(src_ref=src, dst_ref=dst, send_sem=ss, recv_sem=rs,
                                            device_id=place(dev), device_id_type=pl.DeviceIdType.MESH)

    load = pltpu.make_async_copy(qd_h, qd.at[r], loc.at[0])
    load.start()

    barrier = pltpu.get_barrier_semaphore()
    for i in range(1, 8):
        pl.semaphore_signal(barrier, inc=1, device_id=place(lax.rem(me + i, 8)), device_id_type=pl.DeviceIdType.MESH)
    for s in range(2):
        qs[s] = _starts(cu, (2 * chip + s) * C)
    st[r, 0:4] = lse_h[...] * LOG2E
    ones = jnp.ones((8, HD), BF)

    def prepare(h, _):
        x = qd_h[4 + h].astype(F32) * out_h[h].astype(F32)
        hi = x.astype(BF)
        lo = (x - hi.astype(F32)).astype(BF)
        st[r, pl.ds(4 + h, 1)] = (_nt(ones, hi) + _nt(ones, lo))[0:1]
        for s in range(2):
            dq[s, h] = jnp.zeros((HD, C), F32)
        return 0

    lax.fori_loop(0, 4, prepare, 0)
    own[...] = jnp.zeros(own.shape, F32)

    pl.semaphore_wait(barrier, 7)

    q_x = remote(qd_h, qd.at[r], q_send.at[0], q_recv.at[0], mate)
    s_x = remote(st.at[r], st.at[r], q_send.at[1], q_recv.at[1], mate)
    d_x = remote(dq.at[1 - r], dqx, d_send, d_recv, mate)

    own_half = [pltpu.make_async_copy(kv_h[t].at[:, 0], kvr.at[me, t], loc.at[1 + t]) for t in range(2)]
    mate_half = [remote(kv_h[t].at[:, 1], kvr.at[me, t], kv_send.at[0, 1, t], kv_recv.at[me, t], mate) for t in range(2)]

    def keys(tc, par, act):
        for t in range(2):
            act(remote(kv_h[t].at[:, par], kvr.at[me, t], kv_send.at[tc, par, t], kv_recv.at[me, t], 2 * tc + par))

    def keys_via(p, par, act):
        for t in range(2):
            act(remote(kv_h[t].at[:, par], kvx.at[p - 2, t], kv_send.at[2, par, t], x_recv.at[p - 2, t], 6 + par))

    def rank(d, p):
        return lists[d].index(p) if p in lists[d] else 9

    def sends(act):
        for tc in range(1, 4):
            lead = [1 if rank(2 * tc + 1, p) < rank(2 * tc, p) else 0 for p in range(2 * tc)]

            @pl.when((chip < tc) & (me >= lows[tc]))
            def _(tc=tc, lead=lead):
                par0 = _pick(me, lead)
                for par in (par0, 1 - par0):
                    if tc == 2 and key_relay:
                        for p in key_relay:
                            @pl.when(me == p)
                            def _(p=p, par=par):
                                keys_via(p, par, act)

                        @pl.when(chip != 1)
                        def _(par=par):
                            keys(tc, par, act)
                    else:
                        keys(tc, par, act)

    @pl.when(r == 1)
    def _():
        sends(lambda x: x.start())

    q_x.start()

    @pl.when(r == 0)
    def _():
        for x in own_half + mate_half:
            x.start()

    load.wait()
    rows = lax.broadcasted_iota(jnp.int32, (B, B), 0)
    cols = lax.broadcasted_iota(jnp.int32, (B, B), 1)
    frow = lax.broadcasted_iota(jnp.int32, (H, HD), 0)
    frow = frow + lax.div(frow, 128) * 128 + r * 128

    def own_block(kb, _):
        kto[...] = k_h[kb].reshape(B, HD).T

        @pl.when((kb == 1) & (r == 0))
        def _():
            sends(lambda x: x.start())

        def own_tile(qb, _):
            @pl.when((kb == 0) & (qb == 1))
            def _():
                s_x.start()

            q0 = pl.multiple_of(qb * B, B)
            w = pl.ds(q0, B)
            mask = (rows >= qs[r, :, w] - (me * C + kb * B)) & (rows - cols <= q0 - kb * B)
            _tile(k_h[kb].reshape(B, HD), v_h[kb].reshape(B, HD), kto[...], qd, st, mask, None, own.at[0, kb], own.at[1, kb], dq, r, w, B)
            return 0

        lax.fori_loop(kb, C // B, own_tile, 0)
        return 0

    relay_k = [remote(kvx.at[p - 2, t], kvr.at[p, t], x_send.at[p - 2, t], kv_recv.at[p, t], 4 + r) for p in key_relay for t in range(2)]

    def among(p, pieces):
        return functools.reduce(jnp.logical_or, [p == x for x in pieces])

    def back(p, act):
        rest = True
        for pieces, host in ((grad_sum, 6), (grad_relay, 0)):
            if pieces:
                via = (chip == 2) & among(p, pieces)
                rest = rest & jnp.logical_not(via)

                @pl.when(via)
                def _(host=host):
                    act(remote(part.at[p], gx.at[p - 2], r_send.at[p], g_recv.at[p - 2], host + r))

        @pl.when(rest)
        def _():
            act(remote(part.at[p], ret.at[me], r_send.at[p], r_recv.at[me], p))

    def unit(u):
        p = source(u)

        last = u == units - 1

        @pl.when(u == 0)
        def _():
            if key_relay:
                @pl.when(chip == 3)
                def _():
                    for n, p in enumerate(key_relay):
                        for t in range(2):
                            remote(kvx.at[p - 2, t], kvx.at[p - 2, t], x_send.at[p - 2, t], x_recv.at[p - 2, t], mate).wait_recv()
                            relay_k[2 * n + t].start()
            q_x.wait_recv()
            s_x.wait_recv()

        @pl.when(last & (r == 0))
        def _():
            for x in own_half:
                x.wait()

        @pl.when(jnp.logical_not(last) | (r == 1))
        def _():
            for t in range(2):
                remote(kv_h[t].at[:, 0], kvr.at[p, t], kv_send.at[0, 0, t], kv_recv.at[p, t], mate).wait_recv()

        end = p * C + C - 129 + r * 128
        since = 0
        for i in range(1, cu.shape[0] - 1):
            since = jnp.where(cu[i] <= end, cu[i], since)
        live = frow >= since - p * C
        k = kvr[p, 0].reshape(H, HD).astype(F32)
        kf[...] = jnp.where(live, k, k[H - 1:H]).astype(BF)
        ktf[...] = jnp.where(live, k, 0.0).astype(BF).T
        part[p] = jnp.zeros((2, H, HD), F32)

        def far_tile(qb, _):
            s = lax.div(qb, 2)
            w = pl.ds(pl.multiple_of(lax.rem(qb, 2) * H, 128), H)
            _tile(kf[...], kvr[p, 1].reshape(H, HD), ktf[...], qd, st, None, qs[s, :, w] <= end, part.at[p, 0], part.at[p, 1], dq, s, w, H)
            return 0

        need = 1
        for i in range(1, 4):
            need = need + jnp.where(p >= _pick(chip, [first[4 * c + i] for c in range(4)]), 1, 0)
        lax.fori_loop(jnp.where(last, 2, 0), jnp.where(last, 4, need), far_tile, 0)

        for t in range(2):
            part[p, t] = jnp.where(live, part[p, t], 0.0)

        if grad_sum:
            @pl.when((chip == 3) & among(p, grad_sum))
            def _():
                remote(part.at[0], gx.at[p - 2], r_send.at[0], g_recv.at[p - 2], mate).wait_recv()
                part[p] += gx[p - 2]

        @pl.when(jnp.logical_not(last) | (r == 1))
        def _():
            back(p, lambda x: x.start())

    lax.fori_loop(0, C // B, own_block, 0)

    def step(u, _):
        @pl.when((u == units - 1) & (r == 1))
        def _():
            d_x.start()

        unit(u)
        return 0

    lax.fori_loop(0, units, step, 0)

    @pl.when(r == 0)
    def _():
        d_x.start()

    relay_g = [remote(gx.at[p - 2], ret.at[4 + r], x_send.at[p - 2, 0], r_recv.at[4 + r], p) for p in grad_relay]
    if grad_relay:
        @pl.when(chip == 0)
        def _():
            for p, x in zip(grad_relay, relay_g):
                remote(part.at[0], gx.at[p - 2], r_send.at[0], g_recv.at[p - 2], mate).wait_recv()
                x.start()

    def add(src, d):
        a = pl.ds(pl.multiple_of(lax.rem(d, 2) * 128, 128), 128)
        for t in range(2):
            for i in range(3):
                own[t, i, a, :] += src[d, t, pl.ds(i * 128, 128), :]

    d_x.wait_recv()
    scale = HD ** -0.5

    def finish(i, _):
        w = pl.ds(pl.multiple_of(i * 128, 128), 128)
        x = jnp.stack([((dq[r, h, :, w] + dqx[h, :, w]) * scale).T for h in range(4)], axis=0)
        dq_o[w] = jnp.transpose(x, (1, 0, 2)).astype(BF)
        return 0

    lax.fori_loop(0, C // 128, finish, 0)

    @pl.when(r == 0)
    def _():
        add(part, me)
        remote(part.at[0], ret.at[mate], r_send.at[0], r_recv.at[mate], mate).wait_recv()
        add(ret, mate)

    def collect(d, _):
        come = me >= _pick(lax.div(d, 2), lows)
        if grad_sum:
            come = come & jnp.logical_not(among(me, grad_sum) & ((d == 4) | (d == 5)))

        @pl.when(come)
        def _():
            remote(part.at[0], ret.at[d], r_send.at[0], r_recv.at[d], mate).wait_recv()
            add(ret, d)
        return 0

    lax.fori_loop(2 * chip + 2, 8, collect, 0)

    for x in (q_x, s_x, d_x):
        x.wait_send()

    @pl.when(r == 0)
    def _():
        for x in mate_half:
            x.wait_send()

    sends(lambda x: x.wait_send())
    for relays, host in ((relay_k, 3), (relay_g, 0)):
        if relays:
            @pl.when(chip == host)
            def _(relays=relays):
                for x in relays:
                    x.wait_send()

    def drain(u, _):
        @pl.when((u < units - 1) | (r == 1))
        def _():
            back(source(u), lambda x: x.wait_send())
        return 0

    lax.fori_loop(0, units, drain, 0)


def _call(n, cu, *ops):
    vm = pl.BlockSpec(memory_space=pltpu.VMEM)
    dma = pltpu.SemaphoreType.DMA
    return pl.pallas_call(
        functools.partial(_kernel, PATTERNS[n], ORDERS[n], KEY_RELAY[n], GRAD_SUM[n], GRAD_RELAY[n]),
        out_shape=(jax.ShapeDtypeStruct((C, 4, HD), BF), jax.ShapeDtypeStruct((2, 3, B, HD), F32)),
        in_specs=[pl.BlockSpec(memory_space=pltpu.SMEM)] + [vm] * 5, out_specs=(vm, vm),
        scratch_shapes=[
            pltpu.VMEM((2, 8, C, HD), BF), pltpu.VMEM((2, 8, C), F32), pltpu.VMEM((8, 2, 3, 128, HD), BF),
            pltpu.VMEM((2, 1, C), jnp.int32), pltpu.VMEM((HD, B), BF), pltpu.VMEM((HD, H), BF), pltpu.VMEM((H, HD), BF),
            pltpu.VMEM((2, 4, HD, C), F32), pltpu.VMEM((4, HD, C), F32),
            pltpu.VMEM((8, 2, H, HD), F32), pltpu.VMEM((8, 2, H, HD), F32),
            pltpu.VMEM((2, 2, 3, 128, HD), BF), pltpu.VMEM((2, 2, H, HD), F32),
            dma((2, 2)), dma((2, 2)), dma((2,)), dma((3,)), dma((4, 2, 2)), dma((8, 2)), dma((2,)), dma((2,)), dma((8,)), dma((8,)), dma, dma],
        compiler_params=pltpu.CompilerParams(vmem_limit_bytes=52 * 2 ** 20, collective_id=n, has_side_effects=True),
        name='fused%d' % n)(cu, *ops)


def _which_kernel(cu, o):
    ok = [None] * len(PATTERNS)
    for j in range(1, 16):
        start = 0
        for i in range(1, cu.shape[0] - 1):
            start = jnp.where(cu[i] <= j * H, cu[i], start)
        for n, p in enumerate(PATTERNS):
            if p[j]:
                here = start >= p[j] * C
                ok[n] = here if ok[n] is None else ok[n] & here
    best = jnp.int32(len(PATTERNS) - 1)
    for n in range(len(PATTERNS) - 2, -1, -1):
        best = jnp.where(ok[n], n, best)
    o[0] = best


def _which(cu):
    smem = pl.BlockSpec(memory_space=pltpu.SMEM)
    return pl.pallas_call(_which_kernel, out_shape=jax.ShapeDtypeStruct((1,), jnp.int32),
                          in_specs=[smem], out_specs=smem, name='which')(cu)[0]


def solution(mesh):
    tok = P(AXES, 'hp', None)
    tok2 = P(AXES, 'hp')

    def body(q, k, v, out, dout, lse, cu):
        qd = jnp.concatenate([jnp.transpose(q, (1, 0, 2)), jnp.transpose(dout, (1, 0, 2))], 0)
        ops = (cu, qd, jnp.transpose(out, (1, 0, 2)), lse.T, k.reshape(3, 2, 128, HD), v.reshape(3, 2, 128, HD))
        dq, dkv = lax.switch(_which(cu), [functools.partial(_call, n) for n in range(len(PATTERNS))], *ops)
        dkv = dkv.reshape(2, C, 1, HD)
        return dq, (dkv[0] * HD ** -0.5).astype(BF), dkv[1].astype(BF)

    return jax.shard_map(body, mesh=mesh, in_specs=(tok, tok, tok, tok, tok, tok2, P()), out_specs=(tok, tok, tok), check_vma=False)
```
